256 devices in a mesh: slab: 128 (over z, y, x), feat: 2 (over core).
Axes of the slice: x: 4, y: 4, z: 8, core: 2. Of those that a mesh axis runs over, the one named last changes fastest.
Arguments:
- states: float32 [40, 65536], P(None, ('slab', 'feat')), may hold values from -6 to 6
- inputs: float32 [65536], P(('slab', 'feat')), may hold values from -4 to 4
- targets: float32 [40, 65536], P(None, ('slab', 'feat')), may hold values from -4 to 4
Outputs:
- local_operators: float32 [128, 40, 862], P('slab', 'feat')
- scaled_duals: float32 [128, 40, 862], P('slab', 'feat')
- consensus: float32 [40, 862], P('feat')
- residual_history: float32 [2, 2], replicated
The draws below stay inside these ranges and needn't reach their ends.
All inputs are finite; a program needn't handle non-finite values.
Results may differ from the reference program's by a relative error of at most 0.0003.
Values sent between devices are 32-bit elements; how exact they have to be, the bound alone decides.
A program may use at most 64 MiB of HBM per device.

```python
import jax
import jax.numpy as jnp
from jax import lax

R = 40
ITERS = 2
FEATS = 862
SNAPS = 65536
N_SLAB = 128


def joint_draw(key):
    folded = jax.random.fold_in(key, 9031)
    streams = jax.random.split(folded, 10)
    slab_rows = SNAPS // N_SLAB
    slab_scale = jax.random.uniform(streams[0], (N_SLAB,), minval=0.7, maxval=1.4)
    unit_draw = jnp.clip(jax.random.normal(streams[1], (R, N_SLAB, slab_rows)), -4.0, 4.0)
    states = unit_draw * slab_scale[None, :, None]
    forcing = jnp.clip(jax.random.normal(streams[2], (N_SLAB, slab_rows)), -4.0, 4.0)
    root = R ** 0.5
    linear = jax.random.normal(streams[3], (R, R)) / root
    slab_drift = 0.6 * jax.random.normal(streams[4], (N_SLAB, R, R)) / root
    square_map = 0.3 * jax.random.normal(streams[5], (R, R)) / root
    mixed_map = 0.3 * jax.random.normal(streams[6], (R, R)) / root
    input_gain = jax.random.normal(streams[7], (R,))
    offset = jax.random.normal(streams[8], (R,))
    noise_part = 0.3 * jax.random.normal(streams[9], (R, N_SLAB, slab_rows))
    signal = jnp.einsum('ij,jsk->isk', linear, states)
    signal = signal + jnp.einsum('sij,jsk->isk', slab_drift, states)
    signal = signal + jnp.einsum('ij,jsk->isk', square_map, states * states)
    signal = signal + jnp.einsum('ij,jsk->isk', mixed_map, states * jnp.roll(states, 1, axis=0))
    signal = signal + input_gain[:, None, None] * forcing[None] + offset[:, None, None] + noise_part
    targets = 4.0 * jnp.tanh(signal / 4.0)
    return (states.reshape(R, SNAPS), forcing.reshape(SNAPS), targets.reshape(R, SNAPS))


def draw_states(key, part):
    return joint_draw(key)[0].astype(jnp.float32)


def draw_inputs(key, part):
    return joint_draw(key)[1].astype(jnp.float32)


def draw_targets(key, part):
    return joint_draw(key)[2].astype(jnp.float32)


def setup_inputs(seed: int = 0) -> dict:
    streams_of = jax.random.split(jax.random.key(seed), 4)
    return {
        "states": draw_states(jax.random.fold_in(streams_of[3], 71), 0),
        "inputs": draw_inputs(jax.random.fold_in(streams_of[3], 71), 0),
        "targets": draw_targets(jax.random.fold_in(streams_of[3], 71), 0),
    }


penalty = 1.0

def features(states, inputs):
    reduced = states.shape[0]
    blocks = [states]
    for column in range(reduced):
        blocks.append(states[column:column + 1] * states[column:])
    blocks.append(inputs[None, :])
    blocks.append(jnp.ones_like(inputs)[None, :])
    return jnp.concatenate(blocks, 0)

def reference(states, inputs, targets):
    reduced = states.shape[0]
    slab_rows = states.shape[1] // N_SLAB
    slab_states = states.reshape(reduced, N_SLAB, slab_rows).transpose(1, 0, 2)
    slab_targets = targets.reshape(reduced, N_SLAB, slab_rows).transpose(1, 0, 2)
    slab_inputs = inputs.reshape(N_SLAB, slab_rows)

    def local_solve(packed):
        part_states, part_inputs, part_targets, shifted = packed
        design = features(part_states, part_inputs)
        gram_matrix = jnp.dot(design.astype(jnp.float32), design.T.astype(jnp.float32), precision=lax.Precision.HIGHEST, preferred_element_type=jnp.float32) / slab_rows
        cross = jnp.dot(part_targets.astype(jnp.float32), design.T.astype(jnp.float32), precision=lax.Precision.HIGHEST, preferred_element_type=jnp.float32) / slab_rows
        system = gram_matrix + penalty * jnp.eye(design.shape[0], dtype=jnp.float32)
        return jnp.linalg.solve(system, (cross + penalty * shifted).T).T
    width = FEATS
    consensus = jnp.zeros((reduced, width), jnp.float32)
    duals = jnp.zeros((N_SLAB, reduced, width), jnp.float32)
    primal_list = []
    dual_list = []
    operators = duals
    for sweep in range(ITERS):
        operators = lax.map(local_solve, (slab_states, slab_inputs, slab_targets, consensus[None] - duals))
        updated = lax.optimization_barrier(jnp.sum(operators + duals, 0)) / N_SLAB
        duals = duals + operators - updated[None]
        primal_list.append(jnp.sum(jnp.square(operators - updated[None])))
        dual_list.append(N_SLAB * penalty * penalty * jnp.sum(jnp.square(updated - consensus)))
        consensus = updated
    history = jnp.stack([jnp.stack(primal_list), jnp.stack(dual_list)])
    return (operators, duals, consensus, jnp.sqrt(history / (N_SLAB * reduced * width)))
```

```python
import functools

import jax
import jax.numpy as jnp
from jax import lax
from jax.experimental import pallas as pl
from jax.experimental.pallas import tpu as pltpu
from jax.sharding import PartitionSpec as P

F32, BF16 = jnp.float32, jnp.bfloat16
NN = (((1,), (0,)), ((), ()))
NT = (((1,), (1,)), ((), ()))
TN = (((0,), (0,)), ((), ()))
MESH = pl.DeviceIdType.MESH

R = 40
HALF = 20
FEATS = 862
WIDE = 896
PLANE = 16
DEPTH = 8
N_SLAB = 128
M = 512
MINE = 256
rho = 1.0


def dot(a, b, dims):
    return lax.dot_general(a, b, dims, preferred_element_type=F32)


def two(a):
    high = a.astype(BF16)
    return high, (a - high.astype(F32)).astype(BF16)


def dot3(a, b, dims):
    (ah, al), (bh, bl) = a, b
    return dot(ah, bh, dims) + (dot(ah, bl, dims) + dot(al, bh, dims))


def three(a):
    high = a.astype(BF16).astype(F32)
    rest = a - high
    mid = rest.astype(BF16).astype(F32)
    return high, mid, rest - mid


def stacks(x, u):
    def left_of(h, m, l):
        return [h, h, m, h, l, m]

    def right_of(h, m, l):
        return [h, m, h, l, h, m]

    xs, ss, us = three(x), three(x * x), three(u)
    halves = tuple(0.5 * s for s in ss)
    ends = [jnp.ones_like(u), jnp.zeros_like(u)]
    cat = lambda parts: jnp.concatenate(parts, 0).astype(BF16)
    return (
        cat(left_of(*xs)),
        cat(right_of(*xs)),
        cat(left_of(*halves) + left_of(*us) + ends),
        cat(right_of(*ss) + right_of(*us) + ends),
    )


def kernel_block(a, b):
    g = dot(a[0], b[1], TN)
    return g + dot(a[2], b[3], TN) + 0.5 * (g * g)


def add_diagonal(block):
    row = lax.broadcasted_iota(jnp.int32, block.shape, 0)
    col = lax.broadcasted_iota(jnp.int32, block.shape, 1)
    return block + jnp.where(row == col, rho * M, 0.0)


def invert(load, store, n=128, w=8):
    tiles = n // 8
    lane = lax.broadcasted_iota(jnp.int32, (8, n), 1)
    sub = lax.broadcasted_iota(jnp.int32, (8, n), 0)
    a = [load(t) for t in range(tiles)]
    wt = w // 8
    for j in range(n // w):
        k0 = w * j
        mine = range(wt * j, wt * j + wt)
        rest = [t % tiles for t in range(wt * j + wt, wt * j + tiles)]
        inside = (lane >= k0) & (lane < k0 + w)
        cols = {}
        for group in (list(mine), rest[:wt], rest[wt:]):
            for k in range(w):
                for t in group:
                    cols[t, k] = jnp.broadcast_to(a[t][:, k0 + k:k0 + k + 1], (8, n))
        held = {(t, k): cols[t, k] + 0.0 for t in mine for k in range(w)}
        def row_of(x, i):
            return jnp.broadcast_to(x[i:i + 1, :], (8, n))
        e = {(i, k): row_of(held[wt * j + i // 8, k], i % 8) for k in range(w) for i in range(k, w)}
        rows = [row_of(a[wt * j + i // 8], i % 8) for i in range(w)]
        rows = [jnp.where(inside, (lane == k0 + i).astype(F32), rows[i]) for i in range(w)]
        low = {}
        inv = []
        for k in range(w):
            inv.append(1.0 / e[k, k])
            if k + 1 < w:
                e[k + 1, k + 1] = e[k + 1, k + 1] - (e[k + 1, k] * e[k + 1, k]) * inv[k]
            for i in range(k + 1, w):
                low[i, k] = e[i, k] * inv[k]
            for m in range(k + 1, w):
                for i in range(m, w):
                    if i > k + 1:
                        e[i, m] = e[i, m] - low[i, k] * e[m, k]
            for i in range(k + 1, w):
                rows[i] = rows[i] - low[i, k] * rows[k]
        for k in range(w - 1, -1, -1):
            rows[k] = rows[k] * inv[k]
        for i in range(w - 1, 0, -1):
            for k in range(i):
                rows[k] = rows[k] - low[i, k] * rows[i]
        for t in rest:
            new = jnp.where(inside, 0.0, a[t])
            for k in range(w):
                new = new - cols[t, k] * rows[k]
            a[t] = new
        for t in mine:
            new = rows[8 * (t - wt * j)]
            for i in range(1, 8):
                new = jnp.where(sub == i, rows[8 * (t - wt * j) + i], new)
            a[t] = new
    for t in range(tiles):
        store(t, a[t])


def write_features(phi_ref, x_ref, u, at):
    cols = pl.ds(at, MINE)
    phi_ref[0:R, cols] = x_ref[...]
    off = R
    for i in range(R):
        phi_ref[off:off + R - i, cols] = x_ref[i:i + 1, :] * x_ref[i:R, :]
        off += R - i
    phi_ref[off:off + 1, cols] = u
    phi_ref[off + 1:off + 2, cols] = jnp.ones_like(u)
    phi_ref[off + 2:WIDE, cols] = jnp.zeros((WIDE - FEATS, MINE), F32)


def to_chunks(whole, main_ref, ext_ref):
    def piece(r, n, c):
        return whole[r:r + n, 128 * c:128 * c + 128]

    for c in range(7):
        main_ref[2 * c] = piece(0, 8, c)
        main_ref[2 * c + 1] = piece(8, 8, c)
    main_ref[14] = jnp.concatenate([piece(16, 4, 0), piece(16, 4, 1)], 0)
    main_ref[15] = jnp.concatenate([piece(16, 4, 2), piece(16, 4, 3)], 0)
    for i in range(12):
        ext_ref[i] = piece(16 + i % 4, 1, 4 + i // 4)
    for i in range(12, 16):
        ext_ref[i] = jnp.zeros((1, 128), F32)


def from_chunks(main_ref, ext_ref):
    columns = []
    for c in range(7):
        if c < 4:
            last = main_ref[14 + c // 2][4 * (c % 2):4 * (c % 2) + 4, :]
        else:
            last = jnp.concatenate([ext_ref[4 * (c - 4) + i] for i in range(4)], 0)
        columns.append(jnp.concatenate([main_ref[2 * c], main_ref[2 * c + 1], last], 0))
    return jnp.concatenate(columns, 1)


def rows_sum(main, ext):
    return jnp.sum(main, 0, keepdims=True) + ext


def kernel(
    x_ref, u_ref, t_ref, lo_ref, du_ref, co_ref, rh_ref,
    xo, uo, to, phi, phi_h, phi_l, s_ref, d_ref, p_ref, b_h, b_l, l1_ref,
    out_main, out_ext, in_main, in_ext, mid_main, mid_ext, z_main, z_ext, res,
    pair_sems, send1, recv1, send2, recv2, send3, recv3, send_res, recv_res,
):
    slab = lax.axis_index("slab")
    feat = lax.axis_index("feat")
    plane = lax.rem(slab, PLANE)
    depth = lax.div(slab, PLANE)
    other = 1 - feat

    def in_plane(i):
        return depth * PLANE + i

    def in_depth(i):
        return i * PLANE + plane

    barrier = pltpu.get_barrier_semaphore()

    def greet(s, f):
        pl.semaphore_signal(barrier, inc=1, device_id=(s, f), device_id_type=MESH)

    def greet_plane(d, carry):
        peer = in_plane(lax.rem(plane + d, PLANE))
        greet(peer, feat)
        greet(peer, other)
        return carry

    def greet_depth(d, carry):
        greet(in_depth(lax.rem(depth + d, DEPTH)), feat)
        return carry

    greet(slab, other)
    lax.fori_loop(1, PLANE, greet_plane, 0)
    lax.fori_loop(1, DEPTH, greet_depth, 0)

    u_own = u_ref[...]
    own = stacks(x_ref[...], u_own)
    s_ref[0:MINE, 0:MINE] = add_diagonal(kernel_block(own, own))
    write_features(phi, x_ref, u_own, 0)

    pl.semaphore_wait(barrier, 2 * (PLANE - 1) + DEPTH)
    pair = [
        pltpu.make_async_remote_copy(
            src_ref=src, dst_ref=dst, send_sem=pair_sems.at[i], recv_sem=pair_sems.at[3 + i],
            device_id=(slab, other), device_id_type=MESH,
        )
        for i, (src, dst) in enumerate(((x_ref, xo), (u_ref, uo), (t_ref, to)))
    ]
    for copy in pair:
        copy.start()

    def eliminate(kb, carry):
        rows = pl.ds(pl.multiple_of(kb * 128, 128), 128)
        d_ref[...] = s_ref[rows, rows]
        invert(lambda t: d_ref[8 * t:8 * t + 8, :], lambda t, v: d_ref.__setitem__((slice(8 * t, 8 * t + 8), slice(None)), v))

        @pl.when(kb == 0)
        def _():
            for copy in pair:
                copy.wait()
            u_far = uo[...]
            mine = stacks(x_ref[...], u_ref[...])
            far = stacks(xo[...], u_far)
            s_ref[0:MINE, MINE:M] = kernel_block(mine, far)
            s_ref[MINE:M, 0:MINE] = kernel_block(far, mine)
            s_ref[MINE:M, MINE:M] = add_diagonal(kernel_block(far, far))
            write_features(phi, xo, u_far, MINE)

        inverse = d_ref[...]
        p_ref[...] = dot3(two(inverse), two(s_ref[rows, :]), NN)
        p_ref[:, rows] = inverse
        column = two(s_ref[:, rows])
        s_ref[:, rows] = jnp.zeros((M, 128), F32)
        row = two(p_ref[...])
        for rb in range(4):
            part = tuple(c[128 * rb:128 * rb + 128] for c in column)
            s_ref[128 * rb:128 * rb + 128, :] -= dot3(part, row, NN)
        s_ref[rows, :] = p_ref[...]
        return carry

    lax.fori_loop(0, 4, eliminate, 0)

    high, low = two(phi[...])
    phi_h[...] = high
    phi_l[...] = low
    phis = (phi_h, phi_l)

    def with_phi(a, dims):
        return dot3(two(a), (phi_h[...], phi_l[...]), dims)

    first = feat == 0
    targets = jnp.concatenate(
        [jnp.where(first, t[0:HALF, :], t[HALF:R, :]) for t in (t_ref, to)], 1
    )
    inverse = two(s_ref[...])
    w1 = dot3(two(targets), inverse, NN)
    l1 = with_phi(w1, NT)
    l1_ref[...] = l1

    def both(main_src, main_dst, ext_src, ext_dst, send, recv, to_, from_, device):
        return [
            pltpu.make_async_remote_copy(
                src_ref=src, dst_ref=dst, send_sem=send.at[i, to_], recv_sem=recv.at[i, from_],
                device_id=device, device_id_type=MESH,
            )
            for i, (src, dst) in enumerate(((main_src, main_dst), (ext_src, ext_dst)))
        ]

    def scatter(k, peer, at):
        return both(
            out_main.at[k, peer], in_main.at[k, at], out_ext.at[k, peer], in_ext.at[k, at],
            send1.at[k], recv1.at[k], peer, at, (in_plane(peer), feat),
        )

    def across(k, peer, at):
        return both(
            mid_main.at[k, depth], mid_main.at[k, at], mid_ext.at[k, depth], mid_ext.at[k, at],
            send2.at[k], recv2.at[k], peer, at, (in_depth(peer), feat),
        )

    def gather(k, peer, at):
        return both(
            z_main.at[k, plane], z_main.at[k, at], z_ext.at[k, plane], z_ext.at[k, at],
            send3.at[k], recv3.at[k], peer, at, (in_plane(peer), feat),
        )

    def residuals(to_, core, at):
        return pltpu.make_async_remote_copy(
            src_ref=res.at[feat * PLANE + plane], dst_ref=res.at[at],
            send_sem=send_res.at[core * PLANE + to_], recv_sem=recv_res.at[at],
            device_id=(in_plane(to_), core), device_id_type=MESH,
        )

    def start(make, k, me, count):
        def body(d, carry):
            for copy in make(k, lax.rem(me + d, count), me):
                copy.start()
            return carry
        lax.fori_loop(1, count, body, 0)

    def finish(make, k, me, count):
        def body(d, carry):
            peer = lax.rem(me + d, count)
            for copy in make(k, peer, peer):
                copy.wait()
            return carry
        lax.fori_loop(1, count, body, 0)

    def send_chunks(k, whole):
        to_chunks(whole, out_main.at[k], out_ext.at[k])
        start(scatter, k, plane, PLANE)
        in_main[k, plane] = out_main[k, plane]
        in_ext[k, plane] = out_ext[k, plane]

    def squares(pairs, mean):
        total = [jnp.zeros((8, 128), F32), jnp.zeros((1, 128), F32)]
        for piece in pairs:
            for i in range(2):
                gap = piece[i] - mean[i]
                total[i] = total[i] + gap * gap
        return rows_sum(*total)

    def plane_sum(pieces):
        return [functools.reduce(jnp.add, [p[i] for p in pieces]) for i in range(2)]

    def slabs_of(k):
        sent = [(in_main[k, s], in_ext[k, s]) for s in range(PLANE)]
        if k == 0:
            return sent, sent
        before = [(in_main[0, s], in_ext[0, s]) for s in range(PLANE)]
        mean = z_main[0, plane], z_ext[0, plane]
        return sent, [tuple(p - (b - z) for p, b, z in zip(new, old, mean)) for new, old in zip(sent, before)]

    def average(k):
        finish(scatter, k, plane, PLANE)
        sent, operators = slabs_of(k)
        total = plane_sum(sent)
        mean = total if k == 0 else plane_sum(operators)
        mid_main[k, depth] = total[0]
        mid_ext[k, depth] = jnp.concatenate(
            [total[1], squares(operators, [m / PLANE for m in mean])], 0
        )
        start(across, k, depth, DEPTH)

    def conclude(k):
        finish(across, k, depth, DEPTH)
        sums = [(mid_main[k, z], mid_ext[k, z][0:1, :]) for z in range(DEPTH)]
        mean = [m / N_SLAB for m in plane_sum(sums)]
        z_main[k, plane] = mean[0]
        z_ext[k, plane] = mean[1]
        start(gather, k, plane, PLANE)
        if k == 0:
            layers, last = sums, [jnp.zeros((8, 128), F32), jnp.zeros((1, 128), F32)]
        else:
            last = [z_main[0, plane], z_ext[0, plane]]
            old = [(mid_main[0, z], mid_ext[0, z][0:1, :]) for z in range(DEPTH)]
            layers = [tuple(p - (b - PLANE * m) for p, b, m in zip(new, before, last)) for new, before in zip(sums, old)]
        primal = PLANE * squares([tuple(p / PLANE for p in layer) for layer in layers], mean)
        for z in range(DEPTH):
            primal = primal + mid_ext[k, z][1:2, :]
        dual = N_SLAB * rho * rho * squares([mean], last)
        return jnp.sum(primal, 1, keepdims=True), jnp.sum(dual, 1, keepdims=True)

    send_chunks(0, l1)
    rest = two(w1 - rho * M * dot3(two(w1), inverse, NN))
    fixed = dot3(rest, (phi_h[...], phi_l[...]), NT)
    average(0)
    high, low = two(dot3(inverse, (phi_h[...], phi_l[...]), NT))
    b_h[...] = high
    b_l[...] = low
    primal1, dual1 = conclude(0)
    finish(gather, 0, plane, PLANE)
    z1 = from_chunks(z_main.at[0], z_ext.at[0])
    y = two(with_phi(z1, NN))
    l2 = 2.0 * z1 + (fixed - 2.0 * dot3(y, (b_h[...], b_l[...]), NN))
    u1 = l1_ref[...] - z1
    send_chunks(1, l2 + u1)
    lo_ref[0] = l2[:, 0:FEATS]
    u2 = u1 + l2
    average(1)
    primal2, dual2 = conclude(1)
    lane = lax.broadcasted_iota(jnp.int32, (1, 128), 1)
    packed = jnp.zeros((1, 128), F32)
    for i, v in enumerate((primal1, primal2, dual1, dual2)):
        packed = jnp.where(lane == i, v, packed)
    spot = feat * PLANE + plane
    res[spot] = packed
    residuals(plane, other, spot).start()

    def send_residuals(d, carry):
        peer = lax.rem(plane + d, PLANE)
        residuals(peer, feat, spot).start()
        residuals(peer, other, spot).start()
        return carry

    lax.fori_loop(1, PLANE, send_residuals, 0)
    finish(gather, 1, plane, PLANE)
    z2 = from_chunks(z_main.at[1], z_ext.at[1])
    du_ref[0] = (u2 - z2)[:, 0:FEATS]
    co_ref[...] = z2[:, 0:FEATS]
    residuals(plane, other, other * PLANE + plane).wait()

    def wait_residuals(d, carry):
        peer = lax.rem(plane + d, PLANE)
        residuals(peer, feat, feat * PLANE + peer).wait()
        residuals(peer, other, other * PLANE + peer).wait()
        return carry

    lax.fori_loop(1, PLANE, wait_residuals, 0)
    total = functools.reduce(jnp.add, [res[i] for i in range(2 * PLANE)])
    total = jnp.sqrt(total / (N_SLAB * R * FEATS))
    rh_ref[...] = jnp.concatenate([total[:, 0:2], total[:, 2:4]], 0)


def shards(states, inputs, targets):
    vmem = pl.BlockSpec(memory_space=pltpu.VMEM)
    dma = pltpu.SemaphoreType.DMA
    f32 = lambda *shape: pltpu.VMEM(shape, F32)
    half = lambda *shape: pltpu.VMEM(shape, BF16)
    return pl.pallas_call(
        kernel,
        out_shape=(
            jax.ShapeDtypeStruct((1, HALF, FEATS), F32),
            jax.ShapeDtypeStruct((1, HALF, FEATS), F32),
            jax.ShapeDtypeStruct((HALF, FEATS), F32),
            jax.ShapeDtypeStruct((2, 2), F32),
        ),
        in_specs=[vmem] * 3,
        out_specs=(vmem,) * 4,
        scratch_shapes=[
            f32(R, MINE), f32(1, MINE), f32(R, MINE),
            f32(WIDE, M), half(WIDE, M), half(WIDE, M), f32(M, M), f32(128, 128), f32(128, M),
            half(M, WIDE), half(M, WIDE), f32(HALF, WIDE),
            f32(2, PLANE, 8, 128), f32(2, PLANE, 1, 128), f32(2, PLANE, 8, 128), f32(2, PLANE, 1, 128),
            f32(2, DEPTH, 8, 128), f32(2, DEPTH, 2, 128),
            f32(2, PLANE, 8, 128), f32(2, PLANE, 1, 128), f32(2 * PLANE, 1, 128),
            dma((6,)), dma((2, 2, PLANE)), dma((2, 2, PLANE)), dma((2, 2, DEPTH)), dma((2, 2, DEPTH)),
            dma((2, 2, PLANE)), dma((2, 2, PLANE)), dma((2 * PLANE,)), dma((2 * PLANE,)),
        ],
        compiler_params=pltpu.CompilerParams(
            collective_id=0, has_side_effects=True, vmem_limit_bytes=48 * 1024 * 1024
        ),
        name="consensus",
    )(states, inputs.reshape(1, MINE), targets)


def solution(mesh):
    return jax.shard_map(
        shards,
        mesh=mesh,
        in_specs=(P(None, ("slab", "feat")), P(("slab", "feat")), P(None, ("slab", "feat"))),
        out_specs=(P("slab", "feat", None), P("slab", "feat", None), P("feat", None), P()),
        check_vma=False,
    )
```

```python
import functools

import jax
import jax.numpy as jnp
from jax import lax
from jax.experimental import pallas as pl
from jax.experimental.pallas import tpu as pltpu
from jax.sharding import PartitionSpec as P

F32, BF16 = jnp.float32, jnp.bfloat16
NN = (((1,), (0,)), ((), ()))
NT = (((1,), (1,)), ((), ()))
TN = (((0,), (0,)), ((), ()))
MESH = pl.DeviceIdType.MESH

R = 40
HALF = 20
FEATS = 862
WIDE = 896
PLANE = 16
DEPTH = 8
N_SLAB = 128
M = 512
MINE = 256
rho = 1.0


def dot(a, b, dims):
    return lax.dot_general(a, b, dims, preferred_element_type=F32)


def two(a):
    high = a.astype(BF16)
    return high, (a - high.astype(F32)).astype(BF16)


def dot3(a, b, dims):
    (ah, al), (bh, bl) = a, b
    return dot(ah, bh, dims) + (dot(ah, bl, dims) + dot(al, bh, dims))


def three(a):
    high = a.astype(BF16).astype(F32)
    rest = a - high
    mid = rest.astype(BF16).astype(F32)
    return high, mid, rest - mid


def stacks(x, u):
    def left_of(h, m, l):
        return [h, h, m, h, l, m]

    def right_of(h, m, l):
        return [h, m, h, l, h, m]

    xs, ss, us = three(x), three(x * x), three(u)
    halves = tuple(0.5 * s for s in ss)
    ends = [jnp.ones_like(u), jnp.zeros_like(u)]
    cat = lambda parts: jnp.concatenate(parts, 0).astype(BF16)
    return (
        cat(left_of(*xs)),
        cat(right_of(*xs)),
        cat(left_of(*halves) + left_of(*us) + ends),
        cat(right_of(*ss) + right_of(*us) + ends),
    )


def kernel_block(a, b):
    g = dot(a[0], b[1], TN)
    return g + dot(a[2], b[3], TN) + 0.5 * (g * g)


def add_diagonal(block):
    row = lax.broadcasted_iota(jnp.int32, block.shape, 0)
    col = lax.broadcasted_iota(jnp.int32, block.shape, 1)
    return block + jnp.where(row == col, rho * M, 0.0)


def invert(load, store, n=128, w=8):
    tiles, wt = n // 8, w // 8
    lane = lax.broadcasted_iota(jnp.int32, (8, n), 1)
    sub = lax.broadcasted_iota(jnp.int32, (8, n), 0)

    def row_of(x, i):
        return jnp.broadcast_to(x[i:i + 1, :], (8, n))

    a = [load(t) for t in range(tiles)]
    for j in range(n // w):
        k0, t0 = w * j, wt * j
        rest = [t % tiles for t in range(t0 + wt, t0 + tiles)]
        inside = (lane >= k0) & (lane < k0 + w)

        def spread(t, k):
            return jnp.broadcast_to(a[t][:, k0 + k:k0 + k + 1], (8, n))

        spreads = {}
        for group in (range(t0, t0 + wt), rest):
            for k in range(w):
                for t in group:
                    spreads[t, k] = spread(t, k)
        col = [[spreads[t0 + s, k] + 0.0 for s in range(wt)] for k in range(w)]
        row = [jnp.where(inside, (lane == k0 + 8 * s + sub).astype(F32), a[t0 + s]) for s in range(wt)]
        scale = [None] * wt
        for k in range(w):
            s0, i = divmod(k, 8)
            inv = 1.0 / row_of(col[k][s0], i)
            scale[s0] = inv if i == 0 else jnp.where(sub == i, inv, scale[s0])
            off = list(col[k])
            off[s0] = jnp.where(sub == i, 0.0, off[s0])
            for m in range(k + 1, w):
                factor = row_of(col[m][s0], i) * inv
                col[m] = [c - o * factor for c, o in zip(col[m], off)]
            factor = row_of(row[s0], i) * inv
            row = [r - o * factor for r, o in zip(row, off)]
        row = [r * s for r, s in zip(row, scale)]
        pivots = [row_of(row[k // 8], k % 8) for k in range(w)]
        for t in rest:
            new = jnp.where(inside, 0.0, a[t])
            for k in range(w):
                new = new - spreads[t, k] * pivots[k]
            a[t] = new
        for s in range(wt):
            a[t0 + s] = row[s]
    for t in range(tiles):
        store(t, a[t])


def write_features(phi_ref, x_ref, u, at):
    cols = pl.ds(at, MINE)
    phi_ref[0:R, cols] = x_ref[...]
    off = R
    for i in range(R):
        phi_ref[off:off + R - i, cols] = x_ref[i:i + 1, :] * x_ref[i:R, :]
        off += R - i
    phi_ref[off:off + 1, cols] = u
    phi_ref[off + 1:off + 2, cols] = jnp.ones_like(u)
    phi_ref[off + 2:WIDE, cols] = jnp.zeros((WIDE - FEATS, MINE), F32)


def to_chunks(whole, out_ref):
    def piece(r, n, c):
        return whole[r:r + n, 128 * c:128 * c + 128]

    for c in range(7):
        out_ref[2 * c, 0:8, :] = piece(0, 8, c)
        out_ref[2 * c + 1, 0:8, :] = piece(8, 8, c)
    out_ref[14, 0:8, :] = jnp.concatenate([piece(16, 4, 0), piece(16, 4, 1)], 0)
    out_ref[15, 0:8, :] = jnp.concatenate([piece(16, 4, 2), piece(16, 4, 3)], 0)
    for i in range(12):
        out_ref[i, 8:9, :] = piece(16 + i % 4, 1, 4 + i // 4)
    for i in range(12, 16):
        out_ref[i, 8:9, :] = jnp.zeros((1, 128), F32)


def from_chunks(ref):
    columns = []
    for c in range(7):
        if c < 4:
            last = ref[14 + c // 2, 4 * (c % 2):4 * (c % 2) + 4, :]
        else:
            last = jnp.concatenate([ref[4 * (c - 4) + i, 8:9, :] for i in range(4)], 0)
        columns.append(jnp.concatenate([ref[2 * c, 0:8, :], ref[2 * c + 1, 0:8, :], last], 0))
    return jnp.concatenate(columns, 1)


def rows_sum(main, ext):
    return jnp.sum(main, 0, keepdims=True) + ext


def kernel(
    x_ref, u_ref, t_ref, lo_ref, du_ref, co_ref, rh_ref,
    xo, uo, to, phi, phi_h, phi_l, s_ref, d_ref, p_ref, b_h, b_l, l1_ref,
    outs, ins, mids, zs, zs_far, res, sent, stats,
    pair_sems, send1, recv1, send2, recv2, send3, recv3, send_res, recv_res,
):
    slab = lax.axis_index("slab")
    feat = lax.axis_index("feat")
    plane = lax.rem(slab, PLANE)
    depth = lax.div(slab, PLANE)
    line, spot = lax.div(plane, 4), lax.rem(plane, 4)
    other = 1 - feat
    owner = feat == 1
    steps = sorted(((dy, dx) for dy in range(4) for dx in range(4) if dy or dx), key=lambda d: -sum(min(v, 4 - v) for v in d))
    far_planes = [4 * lax.rem(line + dy, 4) + lax.rem(spot + dx, 4) for dy, dx in steps]
    far_depths = [lax.rem(depth + d, DEPTH) for d in (4, 3, 5, 2, 6, 1, 7)]

    def in_plane(i):
        return depth * PLANE + i

    def in_depth(i):
        return i * PLANE + plane

    barrier = pltpu.get_barrier_semaphore()

    def greet(s, f):
        pl.semaphore_signal(barrier, inc=1, device_id=(s, f), device_id_type=MESH)

    greet(slab, other)
    for peer in far_planes:
        greet(in_plane(peer), 1)

    @pl.when(owner)
    def _():
        for peer in far_planes:
            greet(in_plane(peer), 0)
        for peer in far_depths:
            greet(in_depth(peer), 1)

    u_own = u_ref[...]
    own = stacks(x_ref[...], u_own)
    s_ref[0:MINE, 0:MINE] = add_diagonal(kernel_block(own, own))
    write_features(phi, x_ref, u_own, 0)

    pl.semaphore_wait(barrier, PLANE + feat * (PLANE + DEPTH - 2))
    pair = [
        pltpu.make_async_remote_copy(
            src_ref=src, dst_ref=dst, send_sem=pair_sems.at[i], recv_sem=pair_sems.at[3 + i],
            device_id=(slab, other), device_id_type=MESH,
        )
        for i, (src, dst) in enumerate(((x_ref, xo), (u_ref, uo), (t_ref, to)))
    ]
    for copy in pair:
        copy.start()

    def eliminate(kb, carry):
        rows = pl.ds(pl.multiple_of(kb * 128, 128), 128)
        d_ref[...] = s_ref[rows, rows]
        invert(lambda t: d_ref[8 * t:8 * t + 8, :], lambda t, v: d_ref.__setitem__((slice(8 * t, 8 * t + 8), slice(None)), v))

        @pl.when(kb == 0)
        def _():
            for copy in pair:
                copy.wait()
            u_far = uo[...]
            mine = stacks(x_ref[...], u_ref[...])
            far = stacks(xo[...], u_far)
            s_ref[0:MINE, MINE:M] = kernel_block(mine, far)
            s_ref[MINE:M, 0:MINE] = kernel_block(far, mine)
            s_ref[MINE:M, MINE:M] = add_diagonal(kernel_block(far, far))
            write_features(phi, xo, u_far, MINE)

        inverse = d_ref[...]
        p_ref[...] = dot3(two(inverse), two(s_ref[rows, :]), NN)
        p_ref[:, rows] = inverse
        column = two(s_ref[:, rows])
        s_ref[:, rows] = jnp.zeros((M, 128), F32)
        row = two(p_ref[...])
        for rb in range(4):
            part = tuple(c[128 * rb:128 * rb + 128] for c in column)
            s_ref[128 * rb:128 * rb + 128, :] -= dot3(part, row, NN)
        s_ref[rows, :] = p_ref[...]
        return carry

    lax.fori_loop(0, 4, eliminate, 0)

    high, low = two(phi[...])
    phi_h[...] = high
    phi_l[...] = low
    phis = (phi_h, phi_l)

    def with_phi(a, dims):
        return dot3(two(a), (phi_h[...], phi_l[...]), dims)

    first = feat == 0
    targets = jnp.concatenate(
        [jnp.where(first, t[0:HALF, :], t[HALF:R, :]) for t in (t_ref, to)], 1
    )
    inverse = two(s_ref[...])
    w1 = dot3(two(targets), inverse, NN)
    l1 = with_phi(w1, NT)
    l1_ref[...] = l1

    def remote(src, dst, send, recv, device):
        return pltpu.make_async_remote_copy(
            src_ref=src, dst_ref=dst, send_sem=send, recv_sem=recv, device_id=device, device_id_type=MESH
        )

    def take(ref, sem):
        pltpu.make_async_copy(ref, ref, sem).wait()

    def send_chunks(k, whole):
        to_chunks(whole, outs.at[k])

        def scatter(peer):
            remote(
                outs.at[k, peer], ins.at[k, feat * PLANE + plane], send1.at[k], recv1.at[k], (in_plane(peer), 1)
            ).start()

        for peer in far_planes:
            scatter(peer)

        @pl.when(owner)
        def _():
            ins[k, PLANE + plane] = outs[k, plane]

        @pl.when(jnp.logical_not(owner))
        def _():
            scatter(plane)

    def parts(ref, *at):
        return [ref[(*at, slice(0, 8))], ref[(*at, slice(8, 9))]]

    def add_up(pieces):
        return [functools.reduce(jnp.add, [p[i] for p in pieces]) for i in range(2)]

    def squares(pieces, mean):
        total = [jnp.zeros((8, 128), F32), jnp.zeros((1, 128), F32)]
        for piece in pieces:
            for i in range(2):
                gap = piece[i] - mean[i]
                total[i] = total[i] + gap * gap
        return jnp.sum(total[0], 0, keepdims=True) + total[1]

    def consensus_of(k, half):
        return parts(zs, k, plane) if half else parts(zs_far, k)

    def layer(k, z, half):
        return [mids[k, z, 8 * half:8 * half + 8, :], mids[k, z, 16 + half:17 + half, :]]

    def average(k):
        take(ins.at[k, 0:2 * PLANE - 1], recv1.at[k])
        spread = jnp.zeros((1, 128), F32)
        for half in range(2):
            sent = [parts(ins, k, PLANE * half + s) for s in range(PLANE)]
            total = mean = add_up(sent)
            operators = sent
            if k == 1:
                last = consensus_of(0, half)
                before = [parts(ins, 0, PLANE * half + s) for s in range(PLANE)]
                operators = [[p - (b - z) for p, b, z in zip(new, old, last)] for new, old in zip(sent, before)]
                mean = add_up(operators)
            mids[k, depth, 8 * half:8 * half + 8, :] = total[0]
            mids[k, depth, 16 + half:17 + half, :] = total[1]
            spread = spread + squares(operators, [m / PLANE for m in mean])
        mids[k, depth, 18:19, :] = spread
        for peer in far_depths:
            remote(
                mids.at[k, depth], mids.at[k, depth], send2.at[k], recv2.at[k], (in_depth(peer), 1)
            ).start()

    def conclude(k):
        take(mids.at[k, 0:DEPTH - 1], recv2.at[k])
        means = []
        for half in range(2):
            means.append([m / N_SLAB for m in add_up([layer(k, z, half) for z in range(DEPTH)])])
        zs_far[k, 0:8, :] = means[0][0]
        zs_far[k, 8:9, :] = means[0][1]
        zs[k, plane, 0:8, :] = means[1][0]
        zs[k, plane, 8:9, :] = means[1][1]

        def gather(src, peer, core):
            remote(src, zs.at[k, plane], send3.at[k], recv3.at[k], (in_plane(peer), core)).start()

        for peer in far_planes:
            gather(zs_far.at[k], peer, 0)
            gather(zs.at[k, plane], peer, 1)
        gather(zs_far.at[k], plane, 0)

    def statistics(k):
        primal = jnp.zeros((1, 128), F32)
        dual = jnp.zeros((1, 128), F32)
        for half in range(2):
            mean = consensus_of(k, half)
            layers = [layer(k, z, half) for z in range(DEPTH)]
            if k == 0:
                last = [jnp.zeros((8, 128), F32), jnp.zeros((1, 128), F32)]
            else:
                last = consensus_of(0, half)
                before = [layer(0, z, half) for z in range(DEPTH)]
                layers = [[p - (b - PLANE * z) for p, b, z in zip(new, old, last)] for new, old in zip(layers, before)]
            primal = primal + PLANE * squares([[p / PLANE for p in each] for each in layers], mean)
            dual = dual + squares([mean], last)
        for z in range(DEPTH):
            primal = primal + mids[k, z, 18:19, :]
        return jnp.sum(primal, 1, keepdims=True), N_SLAB * rho * rho * jnp.sum(dual, 1, keepdims=True)

    def gathered(k):
        @pl.when(owner)
        def _():
            take(zs.at[k, 0:PLANE - 1], recv3.at[k])

        @pl.when(jnp.logical_not(owner))
        def _():
            take(zs.at[k], recv3.at[k])

        return from_chunks(zs.at[k])

    lane = lax.broadcasted_iota(jnp.int32, (1, 128), 1)

    send_chunks(0, l1)
    rest = two(w1 - rho * M * dot3(two(w1), inverse, NN))
    fixed = dot3(rest, (phi_h[...], phi_l[...]), NT)

    @pl.when(owner)
    def _():
        average(0)

    high, low = two(dot3(inverse, (phi_h[...], phi_l[...]), NT))
    b_h[...] = high
    b_l[...] = low

    @pl.when(owner)
    def _():
        conclude(0)
        primal, dual = statistics(0)
        stats[...] = jnp.where(lane == 0, primal, jnp.where(lane == 2, dual, 0.0))

    z1 = gathered(0)
    y = two(with_phi(z1, NN))
    l2 = 2.0 * z1 + (fixed - 2.0 * dot3(y, (b_h[...], b_l[...]), NN))
    u1 = l1_ref[...] - z1
    send_chunks(1, l2 + u1)
    lo_ref[0] = l2[:, 0:FEATS]
    l1_ref[...] = u1 + l2

    @pl.when(owner)
    def _():
        average(1)
        conclude(1)
        primal, dual = statistics(1)
        res[plane] = jnp.where(lane == 1, primal, jnp.where(lane == 3, dual, stats[...]))
        for peer in far_planes:
            for core in range(2):
                remote(res.at[plane], res.at[plane], send_res.at[0], recv_res.at[0], (in_plane(peer), core)).start()
        remote(res.at[plane], res.at[plane], send_res.at[0], recv_res.at[0], (slab, 0)).start()

    z2 = gathered(1)
    du_ref[0] = (l1_ref[...] - z2)[:, 0:FEATS]
    co_ref[...] = z2[:, 0:FEATS]

    @pl.when(owner)
    def _():
        take(res.at[0:PLANE - 1], recv_res.at[0])

    @pl.when(jnp.logical_not(owner))
    def _():
        take(res, recv_res.at[0])

    total = functools.reduce(jnp.add, [res[i] for i in range(PLANE)])
    total = jnp.sqrt(total / (N_SLAB * R * FEATS))
    rh_ref[...] = jnp.concatenate([total[:, 0:2], total[:, 2:4]], 0)

    @pl.when(owner)
    def _():
        for k in range(2):
            take(outs.at[k, 0:PLANE - 1], send1.at[k])
            take(mids.at[k, 0:DEPTH - 1], send2.at[k])
            take(ins.at[k, 0:2 * PLANE - 1], send3.at[k])
        take(sent.at[0:2 * PLANE - 1], send_res.at[0])

    @pl.when(jnp.logical_not(owner))
    def _():
        for k in range(2):
            take(outs.at[k], send1.at[k])


def shards(states, inputs, targets):
    vmem = pl.BlockSpec(memory_space=pltpu.VMEM)
    dma = pltpu.SemaphoreType.DMA
    f32 = lambda *shape: pltpu.VMEM(shape, F32)
    half = lambda *shape: pltpu.VMEM(shape, BF16)
    return pl.pallas_call(
        kernel,
        out_shape=(
            jax.ShapeDtypeStruct((1, HALF, FEATS), F32),
            jax.ShapeDtypeStruct((1, HALF, FEATS), F32),
            jax.ShapeDtypeStruct((HALF, FEATS), F32),
            jax.ShapeDtypeStruct((2, 2), F32),
        ),
        in_specs=[vmem] * 3,
        out_specs=(vmem,) * 4,
        scratch_shapes=[
            f32(R, MINE), f32(1, MINE), f32(R, MINE),
            f32(WIDE, M), half(WIDE, M), half(WIDE, M), f32(M, M), f32(128, 128), f32(128, M),
            half(M, WIDE), half(M, WIDE), f32(HALF, WIDE),
            f32(2, PLANE, 9, 128), f32(2, 2 * PLANE, 9, 128), f32(2, DEPTH, 19, 128),
            f32(2, PLANE, 9, 128), f32(2, 9, 128), f32(PLANE, 1, 128), f32(2 * PLANE, 1, 128), f32(1, 128),
            dma((6,)), dma((2,)), dma((2,)), dma((2,)), dma((2,)), dma((2,)), dma((2,)), dma((1,)), dma((1,)),
        ],
        compiler_params=pltpu.CompilerParams(
            collective_id=0, has_side_effects=True, vmem_limit_bytes=48 * 1024 * 1024
        ),
        name="consensus",
    )(states, inputs.reshape(1, MINE), targets)


def solution(mesh):
    return jax.shard_map(
        shards,
        mesh=mesh,
        in_specs=(P(None, ("slab", "feat")), P(("slab", "feat")), P(None, ("slab", "feat"))),
        out_specs=(P("slab", "feat", None), P("slab", "feat", None), P("feat", None), P()),
        check_vma=False,
    )
```

```python
import functools

import jax
import jax.numpy as jnp
from jax import lax
from jax.experimental import pallas as pl
from jax.experimental.pallas import tpu as pltpu
from jax.sharding import PartitionSpec as P

F32, BF16 = jnp.float32, jnp.bfloat16
NN = (((1,), (0,)), ((), ()))
NT = (((1,), (1,)), ((), ()))
TN = (((0,), (0,)), ((), ()))
MESH = pl.DeviceIdType.MESH

R = 40
HALF = 20
FEATS = 862
WIDE = 896
PLANE = 16
DEPTH = 8
N_SLAB = 128
M = 512
MINE = 256
rho = 1.0


def dot(a, b, dims):
    return lax.dot_general(a, b, dims, preferred_element_type=F32)


def two(a):
    high = a.astype(BF16)
    return high, (a - high.astype(F32)).astype(BF16)


def dot3(a, b, dims):
    (ah, al), (bh, bl) = a, b
    return dot(ah, bh, dims) + (dot(ah, bl, dims) + dot(al, bh, dims))


def rows3(a, b, dims):
    rows, pad = a.shape[0], -a.shape[0] % 8
    if pad:
        a = jnp.concatenate([a, jnp.zeros((pad, a.shape[1]), F32)], 0)
    tall = rows + pad
    high = a.astype(BF16).astype(F32)
    both = jnp.concatenate([high, a - high], 0).astype(BF16)
    first = dot(both, b[0], dims)
    return (first[0:tall] + (first[tall:] + dot(high.astype(BF16), b[1], dims)))[0:rows]


def three(a):
    high = a.astype(BF16).astype(F32)
    rest = a - high
    mid = rest.astype(BF16).astype(F32)
    return high, mid, rest - mid


def stacks(x, u):
    def left_of(h, m, l):
        return [h, h, m, h, l, m]

    def right_of(h, m, l):
        return [h, m, h, l, h, m]

    xs, ss, us = three(x), three(x * x), three(u)
    halves = tuple(0.5 * s for s in ss)
    ends = [jnp.ones_like(u), jnp.zeros_like(u)]
    cat = lambda parts: jnp.concatenate(parts, 0).astype(BF16)
    return (
        cat(left_of(*xs)),
        cat(right_of(*xs)),
        cat(left_of(*halves) + left_of(*us) + ends),
        cat(right_of(*ss) + right_of(*us) + ends),
    )


def kernel_block(a, b):
    g = dot(a[0], b[1], TN)
    return g + dot(a[2], b[3], TN) + 0.5 * (g * g)


def add_diagonal(block):
    row = lax.broadcasted_iota(jnp.int32, block.shape, 0)
    col = lax.broadcasted_iota(jnp.int32, block.shape, 1)
    return block + jnp.where(row == col, rho * M, 0.0)


def invert(a, n=128, w=16):
    tiles, wt = n // 8, w // 8
    lane = lax.broadcasted_iota(jnp.int32, (8, n), 1)
    sub = lax.broadcasted_iota(jnp.int32, (8, n), 0)

    def row_of(x, i):
        return jnp.broadcast_to(x[i:i + 1, :], (8, n))

    a = [a[8 * t:8 * t + 8] for t in range(tiles)]
    for j in range(n // w):
        k0, t0 = w * j, wt * j
        near = [t % tiles for t in range(t0 + wt, t0 + 2 * wt)] if j + 1 < n // w else []
        rest = [t for t in range(tiles) if t not in near and not t0 <= t < t0 + wt]
        inside = (lane >= k0) & (lane < k0 + w)

        def spread(t, k):
            return jnp.broadcast_to(a[t][:, k0 + k:k0 + k + 1], (8, n))

        col = [[spread(t0 + s, k) + 0.0 for s in range(wt)] for k in range(w)]
        ahead = {(t, k): spread(t, k) for k in range(w) for t in near}
        row = [jnp.where(inside, (lane == k0 + 8 * s + sub).astype(F32), a[t0 + s]) for s in range(wt)]
        scale = [None] * wt
        for k in range(w):
            s0, i = divmod(k, 8)
            inv = 1.0 / row_of(col[k][s0], i)
            scale[s0] = inv if i == 0 else jnp.where(sub == i, inv, scale[s0])
            off = list(col[k])
            off[s0] = jnp.where(sub == i, 0.0, off[s0])
            for m in range(k + 1, w):
                factor = row_of(col[m][s0], i)
                if m == k + 1:
                    col[m] = [c - (o * factor) * inv for c, o in zip(col[m], off)]
                else:
                    factor = factor * inv
                    col[m] = [c - o * factor for c, o in zip(col[m], off)]
            factor = row_of(row[s0], i) * inv
            row = [r - o * factor for r, o in zip(row, off)]
        row = [r * s for r, s in zip(row, scale)]
        pivots = [row_of(row[k // 8], k % 8) for k in range(w)] if near else []
        for t in near:
            terms = [ahead[t, k] * pivots[k] for k in range(w)]
            while len(terms) > 1:
                terms = [functools.reduce(jnp.add, terms[i:i + 2]) for i in range(0, len(terms), 2)]
            a[t] = jnp.where(inside, 0.0, a[t]) - terms[0]
        old = jnp.concatenate([a[t] for t in rest], 0)
        old_h, old_l = two(old)
        new_h, new_l = two(jnp.concatenate(row, 0))
        gap = [jnp.zeros((m, n), BF16) for m in (k0, n - k0 - w)]

        def padded(x):
            return jnp.concatenate([p for p in (gap[0], x, gap[1]) if p.shape[0]], 0)

        high, low = padded(new_h), padded(new_l)
        change = dot(jnp.concatenate([old_h, old_l], 1), jnp.concatenate([high, high], 0), NN) + dot(old_h, low, NN)
        for i, t in enumerate(rest):
            a[t] = jnp.where(inside, 0.0, a[t]) - change[8 * i:8 * i + 8]
        for s in range(wt):
            a[t0 + s] = row[s]
    return jnp.concatenate(a, 0)


def write_features(phi_ref, x_ref, u, at):
    cols = pl.ds(at, MINE)
    phi_ref[0:R, cols] = x_ref[...]
    off = R
    for i in range(R):
        phi_ref[off:off + R - i, cols] = x_ref[i:i + 1, :] * x_ref[i:R, :]
        off += R - i
    phi_ref[off:off + 1, cols] = u
    phi_ref[off + 1:off + 2, cols] = jnp.ones_like(u)
    phi_ref[off + 2:WIDE, cols] = jnp.zeros((WIDE - FEATS, MINE), F32)


def to_chunks(whole, out_ref):
    def piece(r, n, c):
        return whole[r:r + n, 128 * c:128 * c + 128]

    for c in range(7):
        out_ref[2 * c, 0:8, :] = piece(0, 8, c)
        out_ref[2 * c + 1, 0:8, :] = piece(8, 8, c)
    out_ref[14, 0:8, :] = jnp.concatenate([piece(16, 4, 0), piece(16, 4, 1)], 0)
    out_ref[15, 0:8, :] = jnp.concatenate([piece(16, 4, 2), piece(16, 4, 3)], 0)
    for i in range(12):
        out_ref[i, 8:9, :] = piece(16 + i % 4, 1, 4 + i // 4)
    for i in range(12, 16):
        out_ref[i, 8:9, :] = jnp.zeros((1, 128), F32)


def from_chunks(ref):
    columns = []
    for c in range(7):
        if c < 4:
            last = ref[14 + c // 2, 4 * (c % 2):4 * (c % 2) + 4, :]
        else:
            last = jnp.concatenate([ref[4 * (c - 4) + i, 8:9, :] for i in range(4)], 0)
        columns.append(jnp.concatenate([ref[2 * c, 0:8, :], ref[2 * c + 1, 0:8, :], last], 0))
    return jnp.concatenate(columns, 1)


def rows_sum(main, ext):
    return jnp.sum(main, 0, keepdims=True) + ext


def kernel(
    x_ref, u_ref, t_ref, lo_ref, du_ref, co_ref, rh_ref,
    xo, uo, to, phi, phi_h, phi_l, s_ref, d_ref, b_h, b_l, l1_ref,
    outs, ins, mids, zs, zs_far, res, sent, stats,
    pair_sems, send1, recv1, send2, recv2, send3, recv3, send_res, recv_res,
):
    slab = lax.axis_index("slab")
    feat = lax.axis_index("feat")
    plane = lax.rem(slab, PLANE)
    depth = lax.div(slab, PLANE)
    line, spot = lax.div(plane, 4), lax.rem(plane, 4)
    other = 1 - feat
    owner = feat == 1
    steps = sorted(((dy, dx) for dy in range(4) for dx in range(4) if dy or dx), key=lambda d: -sum(min(v, 4 - v) for v in d))
    far_planes = [4 * lax.rem(line + dy, 4) + lax.rem(spot + dx, 4) for dy, dx in steps]
    far_depths = [lax.rem(depth + d, DEPTH) for d in (4, 3, 5, 2, 6, 1, 7)]

    def in_plane(i):
        return depth * PLANE + i

    def in_depth(i):
        return i * PLANE + plane

    barrier = pltpu.get_barrier_semaphore()

    def greet(s, f):
        pl.semaphore_signal(barrier, inc=1, device_id=(s, f), device_id_type=MESH)

    greet(slab, other)
    for peer in far_planes:
        greet(in_plane(peer), 1)

    @pl.when(owner)
    def _():
        for peer in far_planes:
            greet(in_plane(peer), 0)
        for peer in far_depths:
            greet(in_depth(peer), 1)

    u_own = u_ref[...]
    own = stacks(x_ref[...], u_own)
    s_ref[0:MINE, 0:MINE] = add_diagonal(kernel_block(own, own))
    write_features(phi, x_ref, u_own, 0)

    pl.semaphore_wait(barrier, PLANE + feat * (PLANE + DEPTH - 2))
    pair = [
        pltpu.make_async_remote_copy(
            src_ref=src, dst_ref=dst, send_sem=pair_sems.at[i], recv_sem=pair_sems.at[3 + i],
            device_id=(slab, other), device_id_type=MESH,
        )
        for i, (src, dst) in enumerate(((x_ref, xo), (u_ref, uo), (t_ref, to)))
    ]
    for copy in pair:
        copy.start()

    def block(r, c):
        return s_ref[128 * r:128 * r + 128, 128 * c:128 * c + 128]

    def next_block(kb, inverse):
        ahead = dot3(inverse, two(block(kb, kb + 1)), NN)
        return block(kb + 1, kb + 1) - dot3(two(block(kb + 1, kb)), two(ahead), NN)

    def eliminate(kb, inverse):
        rows = slice(128 * kb, 128 * kb + 128)
        high = two(inverse)
        pivots = jnp.concatenate(
            [inverse if c == kb else dot3(high, two(block(kb, c)), NN) for c in range(4)], 1
        )
        halves = two(pivots)
        for rb in range(4):
            if rb != kb:
                change = dot3(two(block(rb, kb)), halves, NN)
                s_ref[128 * rb:128 * rb + 128, rows] = jnp.zeros((128, 128), F32)
                s_ref[128 * rb:128 * rb + 128, :] -= change
        s_ref[rows, :] = pivots

    inverse = invert(block(0, 0))
    pivot = next_block(0, two(inverse))
    for copy in pair:
        copy.wait()
    following = invert(pivot)
    u_far = uo[...]
    own = stacks(x_ref[...], u_ref[...])
    far = stacks(xo[...], u_far)
    s_ref[0:MINE, MINE:M] = kernel_block(own, far)
    s_ref[MINE:M, 0:MINE] = kernel_block(far, own)
    s_ref[MINE:M, MINE:M] = add_diagonal(kernel_block(far, far))
    eliminate(0, inverse)
    write_features(phi, xo, u_far, MINE)
    inverse = following

    pivot = next_block(1, two(inverse))
    following = invert(pivot)
    eliminate(1, inverse)
    high, low = two(phi[...])
    phi_h[...] = high
    phi_l[...] = low
    inverse = following

    pivot = next_block(2, two(inverse))
    following = invert(pivot)
    eliminate(2, inverse)
    inverse = following

    def phis():
        return phi_h[...], phi_l[...]

    first = feat == 0
    targets = jnp.concatenate(
        [jnp.where(first, t[0:HALF, :], t[HALF:R, :]) for t in (t_ref, to)], 1
    )
    rest_rows = slice(0, 384)
    done = s_ref[rest_rows, :]
    left = rows3(targets[:, rest_rows], two(done), NN)
    v = targets[:, 384:M] - left[:, 384:M]
    y = jnp.concatenate([left[:, rest_rows], jnp.zeros((HALF, 128), F32)], 1)
    ly = rows3(y, phis(), NT)
    last = two(s_ref[384:M, rest_rows])
    ph, pl_ = phis()
    g3 = two(dot3(last, (ph[:, rest_rows], pl_[:, rest_rows]), NT) + phi[:, 384:M].T)

    vd = rows3(v, two(inverse), NN)
    l1 = ly + rows3(vd, g3, NN)
    l1_ref[...] = l1
    d_ref[...] = inverse

    def remote(src, dst, send, recv, device):
        return pltpu.make_async_remote_copy(
            src_ref=src, dst_ref=dst, send_sem=send, recv_sem=recv, device_id=device, device_id_type=MESH
        )

    def take(ref, sem):
        pltpu.make_async_copy(ref, ref, sem).wait()

    def send_chunks(k, whole):
        to_chunks(whole, outs.at[k])

        def scatter(peer):
            remote(
                outs.at[k, peer], ins.at[k, feat * PLANE + plane], send1.at[k], recv1.at[k], (in_plane(peer), 1)
            ).start()

        for peer in far_planes:
            scatter(peer)

        @pl.when(owner)
        def _():
            ins[k, PLANE + plane] = outs[k, plane]

        @pl.when(jnp.logical_not(owner))
        def _():
            scatter(plane)

    def parts(ref, *at):
        return [ref[(*at, slice(0, 8))], ref[(*at, slice(8, 9))]]

    def add_up(pieces):
        return [functools.reduce(jnp.add, [p[i] for p in pieces]) for i in range(2)]

    def squares(pieces, mean):
        total = [jnp.zeros((8, 128), F32), jnp.zeros((1, 128), F32)]
        for piece in pieces:
            for i in range(2):
                gap = piece[i] - mean[i]
                total[i] = total[i] + gap * gap
        return jnp.sum(total[0], 0, keepdims=True) + total[1]

    def consensus_of(k, half):
        return parts(zs, k, plane) if half else parts(zs_far, k)

    def layer(k, z, half):
        return [mids[k, z, 8 * half:8 * half + 8, :], mids[k, z, 16 + half:17 + half, :]]

    def average(k):
        take(ins.at[k, 0:2 * PLANE - 1], recv1.at[k])
        spread = jnp.zeros((1, 128), F32)
        for half in range(2):
            sent = [parts(ins, k, PLANE * half + s) for s in range(PLANE)]
            total = mean = add_up(sent)
            operators = sent
            if k == 1:
                last = consensus_of(0, half)
                before = [parts(ins, 0, PLANE * half + s) for s in range(PLANE)]
                operators = [[p - (b - z) for p, b, z in zip(new, old, last)] for new, old in zip(sent, before)]
                mean = add_up(operators)
            mids[k, depth, 8 * half:8 * half + 8, :] = total[0]
            mids[k, depth, 16 + half:17 + half, :] = total[1]
            spread = spread + squares(operators, [m / PLANE for m in mean])
        mids[k, depth, 18:19, :] = spread
        for peer in far_depths:
            remote(
                mids.at[k, depth], mids.at[k, depth], send2.at[k], recv2.at[k], (in_depth(peer), 1)
            ).start()

    def conclude(k):
        take(mids.at[k, 0:DEPTH - 1], recv2.at[k])
        means = []
        for half in range(2):
            means.append([m / N_SLAB for m in add_up([layer(k, z, half) for z in range(DEPTH)])])
        zs_far[k, 0:8, :] = means[0][0]
        zs_far[k, 8:9, :] = means[0][1]
        zs[k, plane, 0:8, :] = means[1][0]
        zs[k, plane, 8:9, :] = means[1][1]

        def gather(src, peer, core):
            remote(src, zs.at[k, plane], send3.at[k], recv3.at[k], (in_plane(peer), core)).start()

        for peer in far_planes:
            gather(zs_far.at[k], peer, 0)
            gather(zs.at[k, plane], peer, 1)
        gather(zs_far.at[k], plane, 0)

    def statistics(k):
        primal = jnp.zeros((1, 128), F32)
        dual = jnp.zeros((1, 128), F32)
        for half in range(2):
            mean = consensus_of(k, half)
            layers = [layer(k, z, half) for z in range(DEPTH)]
            if k == 0:
                last = [jnp.zeros((8, 128), F32), jnp.zeros((1, 128), F32)]
            else:
                last = consensus_of(0, half)
                before = [layer(0, z, half) for z in range(DEPTH)]
                layers = [[p - (b - PLANE * z) for p, b, z in zip(new, old, last)] for new, old in zip(layers, before)]
            primal = primal + PLANE * squares([[p / PLANE for p in each] for each in layers], mean)
            dual = dual + squares([mean], last)
        for z in range(DEPTH):
            primal = primal + mids[k, z, 18:19, :]
        return jnp.sum(primal, 1, keepdims=True), N_SLAB * rho * rho * jnp.sum(dual, 1, keepdims=True)

    def gathered(k):
        @pl.when(owner)
        def _():
            take(zs.at[k, 0:PLANE - 1], recv3.at[k])

        @pl.when(jnp.logical_not(owner))
        def _():
            take(zs.at[k], recv3.at[k])

        return from_chunks(zs.at[k])

    lane = lax.broadcasted_iota(jnp.int32, (1, 128), 1)

    send_chunks(0, l1)
    w1 = y + jnp.concatenate([rows3(vd, last, NN), vd], 1)
    eliminate(3, d_ref[...])
    inverse = two(s_ref[...])
    fixed = rows3(w1 - rho * M * rows3(w1, inverse, NN), phis(), NT)

    @pl.when(owner)
    def _():
        average(0)

    high, low = two(dot3(inverse, (phi_h[...], phi_l[...]), NT))
    b_h[...] = high
    b_l[...] = low

    @pl.when(owner)
    def _():
        conclude(0)
        primal, dual = statistics(0)
        stats[...] = jnp.where(lane == 0, primal, jnp.where(lane == 2, dual, 0.0))

    z1 = gathered(0)
    l2 = 2.0 * z1 + (fixed - 2.0 * rows3(rows3(z1, phis(), NN), (b_h[...], b_l[...]), NN))
    u1 = l1_ref[...] - z1
    send_chunks(1, l2 + u1)
    lo_ref[0] = l2[:, 0:FEATS]
    l1_ref[...] = u1 + l2

    @pl.when(owner)
    def _():
        average(1)
        conclude(1)
        primal, dual = statistics(1)
        res[plane] = jnp.where(lane == 1, primal, jnp.where(lane == 3, dual, stats[...]))
        for peer in far_planes:
            for core in range(2):
                remote(res.at[plane], res.at[plane], send_res.at[0], recv_res.at[0], (in_plane(peer), core)).start()
        remote(res.at[plane], res.at[plane], send_res.at[0], recv_res.at[0], (slab, 0)).start()

    z2 = gathered(1)
    du_ref[0] = (l1_ref[...] - z2)[:, 0:FEATS]
    co_ref[...] = z2[:, 0:FEATS]

    @pl.when(owner)
    def _():
        take(res.at[0:PLANE - 1], recv_res.at[0])

    @pl.when(jnp.logical_not(owner))
    def _():
        take(res, recv_res.at[0])

    total = functools.reduce(jnp.add, [res[i] for i in range(PLANE)])
    total = jnp.sqrt(total / (N_SLAB * R * FEATS))
    rh_ref[...] = jnp.concatenate([total[:, 0:2], total[:, 2:4]], 0)

    @pl.when(owner)
    def _():
        for k in range(2):
            take(outs.at[k, 0:PLANE - 1], send1.at[k])
            take(mids.at[k, 0:DEPTH - 1], send2.at[k])
            take(ins.at[k, 0:2 * PLANE - 1], send3.at[k])
        take(sent.at[0:2 * PLANE - 1], send_res.at[0])

    @pl.when(jnp.logical_not(owner))
    def _():
        for k in range(2):
            take(outs.at[k], send1.at[k])


def shards(states, inputs, targets):
    vmem = pl.BlockSpec(memory_space=pltpu.VMEM)
    dma = pltpu.SemaphoreType.DMA
    f32 = lambda *shape: pltpu.VMEM(shape, F32)
    half = lambda *shape: pltpu.VMEM(shape, BF16)
    return pl.pallas_call(
        kernel,
        out_shape=(
            jax.ShapeDtypeStruct((1, HALF, FEATS), F32),
            jax.ShapeDtypeStruct((1, HALF, FEATS), F32),
            jax.ShapeDtypeStruct((HALF, FEATS), F32),
            jax.ShapeDtypeStruct((2, 2), F32),
        ),
        in_specs=[vmem] * 3,
        out_specs=(vmem,) * 4,
        scratch_shapes=[
            f32(R, MINE), f32(1, MINE), f32(R, MINE),
            f32(WIDE, M), half(WIDE, M), half(WIDE, M), f32(M, M), f32(128, 128),
            half(M, WIDE), half(M, WIDE), f32(HALF, WIDE),
            f32(2, PLANE, 9, 128), f32(2, 2 * PLANE, 9, 128), f32(2, DEPTH, 19, 128),
            f32(2, PLANE, 9, 128), f32(2, 9, 128), f32(PLANE, 1, 128), f32(2 * PLANE, 1, 128), f32(1, 128),
            dma((6,)), dma((2,)), dma((2,)), dma((2,)), dma((2,)), dma((2,)), dma((2,)), dma((1,)), dma((1,)),
        ],
        compiler_params=pltpu.CompilerParams(
            collective_id=0, has_side_effects=True, vmem_limit_bytes=48 * 1024 * 1024
        ),
        name="consensus",
    )(states, inputs.reshape(1, MINE), targets)


def solution(mesh):
    return jax.shard_map(
        shards,
        mesh=mesh,
        in_specs=(P(None, ("slab", "feat")), P(("slab", "feat")), P(None, ("slab", "feat"))),
        out_specs=(P("slab", "feat", None), P("slab", "feat", None), P("feat", None), P()),
        check_vma=False,
    )
```

```python
import functools

import jax
import jax.numpy as jnp
from jax import lax
from jax.experimental import pallas as pl
from jax.experimental.pallas import tpu as pltpu
from jax.sharding import PartitionSpec as P

F32, BF16 = jnp.float32, jnp.bfloat16
NN = (((1,), (0,)), ((), ()))
NT = (((1,), (1,)), ((), ()))
TN = (((0,), (0,)), ((), ()))
MESH = pl.DeviceIdType.MESH

R = 40
HALF = 20
FEATS = 862
WIDE = 896
PLANE = 16
DEPTH = 8
N_SLAB = 128
M = 512
MINE = 256
rho = 1.0


def dot(a, b, dims):
    return lax.dot_general(a, b, dims, preferred_element_type=F32)


def two(a):
    high = a.astype(BF16)
    return high, (a - high.astype(F32)).astype(BF16)


def dot3(a, b, dims):
    (ah, al), (bh, bl) = a, b
    return dot(ah, bh, dims) + (dot(ah, bl, dims) + dot(al, bh, dims))


def rows3(a, b, dims):
    rows, pad = a.shape[0], -a.shape[0] % 8
    if pad:
        a = jnp.concatenate([a, jnp.zeros((pad, a.shape[1]), F32)], 0)
    tall = rows + pad
    high = a.astype(BF16).astype(F32)
    both = jnp.concatenate([high, a - high], 0).astype(BF16)
    first = dot(both, b[0], dims)
    return (first[0:tall] + (first[tall:] + dot(high.astype(BF16), b[1], dims)))[0:rows]


def three(a):
    high = a.astype(BF16).astype(F32)
    rest = a - high
    mid = rest.astype(BF16).astype(F32)
    return high, mid, rest - mid


def stacks(x, u):
    def left_of(h, m, l):
        return [h, h, m, h, l, m]

    def right_of(h, m, l):
        return [h, m, h, l, h, m]

    xs, ss, us = three(x), three(x * x), three(u)
    halves = tuple(0.5 * s for s in ss)
    ends = [jnp.ones_like(u), jnp.zeros_like(u)]
    cat = lambda parts: jnp.concatenate(parts, 0).astype(BF16)
    return (
        cat(left_of(*xs)),
        cat(right_of(*xs)),
        cat(left_of(*halves) + left_of(*us) + ends),
        cat(right_of(*ss) + right_of(*us) + ends),
    )


def kernel_block(a, b):
    g = dot(a[0], b[1], TN)
    return g + dot(a[2], b[3], TN) + 0.5 * (g * g)


def add_diagonal(block):
    row = lax.broadcasted_iota(jnp.int32, block.shape, 0)
    col = lax.broadcasted_iota(jnp.int32, block.shape, 1)
    return block + jnp.where(row == col, rho * M, 0.0)


def invert(a, n=128, w=16):
    tiles, wt = n // 8, w // 8
    lane = lax.broadcasted_iota(jnp.int32, (8, n), 1)
    sub = lax.broadcasted_iota(jnp.int32, (8, n), 0)

    def row_of(x, i):
        return jnp.broadcast_to(x[i:i + 1, :], (8, n))

    a = [a[8 * t:8 * t + 8] for t in range(tiles)]
    for j in range(n // w):
        k0, t0 = w * j, wt * j
        near = [t % tiles for t in range(t0 + wt, t0 + 2 * wt)] if j + 1 < n // w else []
        rest = [t for t in range(tiles) if t not in near and not t0 <= t < t0 + wt]
        inside = (lane >= k0) & (lane < k0 + w)

        def spread(t, k):
            return jnp.broadcast_to(a[t][:, k0 + k:k0 + k + 1], (8, n))

        col = [[spread(t0 + s, k) + 0.0 for s in range(wt)] for k in range(w)]
        ahead = {(t, k): spread(t, k) for k in range(w) for t in near}
        row = [jnp.where(inside, (lane == k0 + 8 * s + sub).astype(F32), a[t0 + s]) for s in range(wt)]
        scale = [None] * wt
        for k in range(w):
            s0, i = divmod(k, 8)
            inv = 1.0 / row_of(col[k][s0], i)
            scale[s0] = inv if i == 0 else jnp.where(sub == i, inv, scale[s0])
            off = list(col[k])
            off[s0] = jnp.where(sub == i, 0.0, off[s0])
            for m in range(k + 1, w):
                factor = row_of(col[m][s0], i)
                if m == k + 1:
                    col[m] = [c - (o * factor) * inv for c, o in zip(col[m], off)]
                else:
                    factor = factor * inv
                    col[m] = [c - o * factor for c, o in zip(col[m], off)]
            factor = row_of(row[s0], i) * inv
            row = [r - o * factor for r, o in zip(row, off)]
        row = [r * s for r, s in zip(row, scale)]
        pivots = [row_of(row[k // 8], k % 8) for k in range(w)] if near else []
        for t in near:
            terms = [ahead[t, k] * pivots[k] for k in range(w)]
            while len(terms) > 1:
                terms = [functools.reduce(jnp.add, terms[i:i + 2]) for i in range(0, len(terms), 2)]
            a[t] = jnp.where(inside, 0.0, a[t]) - terms[0]
        old = jnp.concatenate([a[t] for t in rest], 0)
        old_h, old_l = two(old)
        new_h, new_l = two(jnp.concatenate(row, 0))
        gap = [jnp.zeros((m, n), BF16) for m in (k0, n - k0 - w)]

        def padded(x):
            return jnp.concatenate([p for p in (gap[0], x, gap[1]) if p.shape[0]], 0)

        high, low = padded(new_h), padded(new_l)
        change = dot(jnp.concatenate([old_h, old_l], 1), jnp.concatenate([high, high], 0), NN) + dot(old_h, low, NN)
        for i, t in enumerate(rest):
            a[t] = jnp.where(inside, 0.0, a[t]) - change[8 * i:8 * i + 8]
        for s in range(wt):
            a[t0 + s] = row[s]
    return jnp.concatenate(a, 0)


def write_features(phi_ref, x_ref, u, at):
    cols = pl.ds(at, MINE)
    phi_ref[0:R, cols] = x_ref[...]
    off = R
    for i in range(R):
        phi_ref[off:off + R - i, cols] = x_ref[i:i + 1, :] * x_ref[i:R, :]
        off += R - i
    phi_ref[off:off + 1, cols] = u
    phi_ref[off + 1:off + 2, cols] = jnp.ones_like(u)
    phi_ref[off + 2:WIDE, cols] = jnp.zeros((WIDE - FEATS, MINE), F32)


def to_chunks(whole, out_ref):
    def piece(r, n, c):
        return whole[r:r + n, 128 * c:128 * c + 128]

    for c in range(7):
        out_ref[2 * c, 0:8, :] = piece(0, 8, c)
        out_ref[2 * c + 1, 0:8, :] = piece(8, 8, c)
    out_ref[14, 0:8, :] = jnp.concatenate([piece(16, 4, 0), piece(16, 4, 1)], 0)
    out_ref[15, 0:8, :] = jnp.concatenate([piece(16, 4, 2), piece(16, 4, 3)], 0)
    for i in range(12):
        out_ref[i, 8:9, :] = piece(16 + i % 4, 1, 4 + i // 4)
    for i in range(12, 16):
        out_ref[i, 8:9, :] = jnp.zeros((1, 128), F32)


def from_chunks(ref):
    columns = []
    for c in range(7):
        if c < 4:
            last = ref[14 + c // 2, 4 * (c % 2):4 * (c % 2) + 4, :]
        else:
            last = jnp.concatenate([ref[4 * (c - 4) + i, 8:9, :] for i in range(4)], 0)
        columns.append(jnp.concatenate([ref[2 * c, 0:8, :], ref[2 * c + 1, 0:8, :], last], 0))
    return jnp.concatenate(columns, 1)


def rows_sum(main, ext):
    return jnp.sum(main, 0, keepdims=True) + ext


def kernel(
    x_ref, u_ref, t_ref, lo_ref, du_ref, co_ref, rh_ref,
    xo, uo, to, phi, phi_h, phi_l, s_ref, d_ref, b_h, b_l, l1_ref,
    outs, ins, mids, zs, zs_far, res, sent, stats,
    pair_sems, send1, recv1, send2, recv2, send3, recv3, send_res, recv_res,
):
    slab = lax.axis_index("slab")
    feat = lax.axis_index("feat")
    plane = lax.rem(slab, PLANE)
    depth = lax.div(slab, PLANE)
    line, spot = lax.div(plane, 4), lax.rem(plane, 4)
    other = 1 - feat
    owner = feat == 1
    steps = sorted(((dy, dx) for dy in range(4) for dx in range(4) if dy or dx), key=lambda d: -sum(min(v, 4 - v) for v in d))
    far_planes = [4 * lax.rem(line + dy, 4) + lax.rem(spot + dx, 4) for dy, dx in steps]
    far_depths = [lax.rem(depth + d, DEPTH) for d in (4, 3, 5, 2, 6, 1, 7)]

    def in_plane(i):
        return depth * PLANE + i

    def in_depth(i):
        return i * PLANE + plane

    barrier = pltpu.get_barrier_semaphore()

    def greet(s, f):
        pl.semaphore_signal(barrier, inc=1, device_id=(s, f), device_id_type=MESH)

    greet(slab, other)
    for peer in far_planes:
        greet(in_plane(peer), 1)

    @pl.when(owner)
    def _():
        for peer in far_planes:
            greet(in_plane(peer), 0)
        for peer in far_depths:
            greet(in_depth(peer), 1)

    u_own = u_ref[...]
    own = stacks(x_ref[...], u_own)
    s_ref[0:MINE, 0:MINE] = add_diagonal(kernel_block(own, own))
    write_features(phi, x_ref, u_own, 0)

    pl.semaphore_wait(barrier, PLANE + feat * (PLANE + DEPTH - 2))
    pair = [
        pltpu.make_async_remote_copy(
            src_ref=src, dst_ref=dst, send_sem=pair_sems.at[i], recv_sem=pair_sems.at[3 + i],
            device_id=(slab, other), device_id_type=MESH,
        )
        for i, (src, dst) in enumerate(((x_ref, xo), (u_ref, uo), (t_ref, to)))
    ]
    for copy in pair:
        copy.start()

    def block(r, c):
        return s_ref[128 * r:128 * r + 128, 128 * c:128 * c + 128]

    def next_block(kb, inverse):
        ahead = dot3(inverse, two(block(kb, kb + 1)), NN)
        return block(kb + 1, kb + 1) - dot3(two(block(kb + 1, kb)), two(ahead), NN)

    def eliminate(kb, inverse):
        rows = slice(128 * kb, 128 * kb + 128)
        high = two(inverse)
        pivots = jnp.concatenate(
            [inverse if c == kb else dot3(high, two(block(kb, c)), NN) for c in range(4)], 1
        )
        halves = two(pivots)
        for rb in range(4):
            if rb != kb:
                change = dot3(two(block(rb, kb)), halves, NN)
                s_ref[128 * rb:128 * rb + 128, rows] = jnp.zeros((128, 128), F32)
                s_ref[128 * rb:128 * rb + 128, :] -= change
        s_ref[rows, :] = pivots

    inverse = invert(block(0, 0))
    pivot = next_block(0, two(inverse))
    for copy in pair:
        copy.wait()
    following = invert(pivot)
    u_far = uo[...]
    own = stacks(x_ref[...], u_ref[...])
    far = stacks(xo[...], u_far)
    s_ref[0:MINE, MINE:M] = kernel_block(own, far)
    s_ref[MINE:M, 0:MINE] = kernel_block(far, own)
    s_ref[MINE:M, MINE:M] = add_diagonal(kernel_block(far, far))
    eliminate(0, inverse)
    write_features(phi, xo, u_far, MINE)
    inverse = following

    pivot = next_block(1, two(inverse))
    following = invert(pivot)
    eliminate(1, inverse)
    high, low = two(phi[...])
    phi_h[...] = high
    phi_l[...] = low
    inverse = following

    pivot = next_block(2, two(inverse))
    following = invert(pivot)
    eliminate(2, inverse)
    inverse = following

    def phis():
        return phi_h[...], phi_l[...]

    first = feat == 0
    targets = jnp.concatenate(
        [jnp.where(first, t[0:HALF, :], t[HALF:R, :]) for t in (t_ref, to)], 1
    )
    rest_rows = slice(0, 384)
    done = s_ref[rest_rows, :]
    left = rows3(targets[:, rest_rows], two(done), NN)
    v = targets[:, 384:M] - left[:, 384:M]
    y = jnp.concatenate([left[:, rest_rows], jnp.zeros((HALF, 128), F32)], 1)
    ly = rows3(y, phis(), NT)
    last = two(s_ref[384:M, rest_rows])
    ph, pl_ = phis()
    g3 = two(dot3(last, (ph[:, rest_rows], pl_[:, rest_rows]), NT) + phi[:, 384:M].T)

    vd = rows3(v, two(inverse), NN)
    l1 = ly + rows3(vd, g3, NN)
    l1_ref[...] = l1
    d_ref[...] = inverse

    def remote(src, dst, send, recv, device):
        return pltpu.make_async_remote_copy(
            src_ref=src, dst_ref=dst, send_sem=send, recv_sem=recv, device_id=device, device_id_type=MESH
        )

    def take(ref, sem):
        pltpu.make_async_copy(ref, ref, sem).wait()

    def send_chunks(k, whole):
        to_chunks(whole, outs.at[k])

        def scatter(peer):
            remote(
                outs.at[k, peer], ins.at[k, feat * PLANE + plane], send1.at[k], recv1.at[k], (in_plane(peer), 1)
            ).start()

        for peer in far_planes:
            scatter(peer)

        @pl.when(owner)
        def _():
            ins[k, PLANE + plane] = outs[k, plane]

        @pl.when(jnp.logical_not(owner))
        def _():
            scatter(plane)

    def parts(ref, *at):
        return [ref[(*at, slice(0, 8))], ref[(*at, slice(8, 9))]]

    def add_up(pieces):
        return [functools.reduce(jnp.add, [p[i] for p in pieces]) for i in range(2)]

    def squares(pieces, mean):
        total = [jnp.zeros((8, 128), F32), jnp.zeros((1, 128), F32)]
        for piece in pieces:
            for i in range(2):
                gap = piece[i] - mean[i]
                total[i] = total[i] + gap * gap
        return jnp.sum(total[0], 0, keepdims=True) + total[1]

    def consensus_of(k, half):
        return parts(zs, k, plane) if half else parts(zs_far, k)

    def layer(k, z, half):
        return [mids[k, z, 8 * half:8 * half + 8, :], mids[k, z, 16 + half:17 + half, :]]

    def average(k):
        take(ins.at[k, 0:2 * PLANE - 1], recv1.at[k])
        spread = jnp.zeros((1, 128), F32)
        for half in range(2):
            sent = [parts(ins, k, PLANE * half + s) for s in range(PLANE)]
            total = mean = add_up(sent)
            operators = sent
            if k == 1:
                last = consensus_of(0, half)
                before = [parts(ins, 0, PLANE * half + s) for s in range(PLANE)]
                operators = [[p - (b - z) for p, b, z in zip(new, old, last)] for new, old in zip(sent, before)]
                mean = add_up(operators)
            mids[k, depth, 8 * half:8 * half + 8, :] = total[0]
            mids[k, depth, 16 + half:17 + half, :] = total[1]
            spread = spread + squares(operators, [m / PLANE for m in mean])
        mids[k, depth, 18:19, :] = spread
        for peer in far_depths:
            remote(
                mids.at[k, depth], mids.at[k, depth], send2.at[k], recv2.at[k], (in_depth(peer), 1)
            ).start()

    def conclude(k):
        take(mids.at[k, 0:DEPTH - 1], recv2.at[k])
        means = []
        for half in range(2):
            means.append([m / N_SLAB for m in add_up([layer(k, z, half) for z in range(DEPTH)])])
        zs_far[k, 0:8, :] = means[0][0]
        zs_far[k, 8:9, :] = means[0][1]
        zs[k, plane, 0:8, :] = means[1][0]
        zs[k, plane, 8:9, :] = means[1][1]

        def gather(src, peer, core):
            remote(src, zs.at[k, plane], send3.at[k], recv3.at[k], (in_plane(peer), core)).start()

        for peer in far_planes:
            gather(zs_far.at[k], peer, 0)
            gather(zs.at[k, plane], peer, 1)
        gather(zs_far.at[k], plane, 0)

    def statistics(k):
        primal = jnp.zeros((1, 128), F32)
        dual = jnp.zeros((1, 128), F32)
        for half in range(2):
            mean = consensus_of(k, half)
            layers = [layer(k, z, half) for z in range(DEPTH)]
            if k == 0:
                last = [jnp.zeros((8, 128), F32), jnp.zeros((1, 128), F32)]
            else:
                last = consensus_of(0, half)
                before = [layer(0, z, half) for z in range(DEPTH)]
                layers = [[p - (b - PLANE * z) for p, b, z in zip(new, old, last)] for new, old in zip(layers, before)]
            primal = primal + PLANE * squares([[p / PLANE for p in each] for each in layers], mean)
            dual = dual + squares([mean], last)
        for z in range(DEPTH):
            primal = primal + mids[k, z, 18:19, :]
        return jnp.sum(primal, 1, keepdims=True), N_SLAB * rho * rho * jnp.sum(dual, 1, keepdims=True)

    def gathered(k):
        @pl.when(owner)
        def _():
            take(zs.at[k, 0:PLANE - 1], recv3.at[k])

        @pl.when(jnp.logical_not(owner))
        def _():
            take(zs.at[k], recv3.at[k])

        return from_chunks(zs.at[k])

    lane = lax.broadcasted_iota(jnp.int32, (1, 128), 1)

    send_chunks(0, l1)
    w1 = y + jnp.concatenate([rows3(vd, last, NN), vd], 1)
    eliminate(3, d_ref[...])
    inverse = two(s_ref[...])
    fixed = rows3(w1 - rho * M * rows3(w1, inverse, NN), phis(), NT)

    @pl.when(owner)
    def _():
        average(0)

    high, low = two(dot3(inverse, (phi_h[...], phi_l[...]), NT))
    b_h[...] = high
    b_l[...] = low

    @pl.when(owner)
    def _():
        conclude(0)
        primal, dual = statistics(0)
        stats[...] = jnp.where(lane == 0, primal, jnp.where(lane == 2, dual, 0.0))

    z1 = gathered(0)
    l2 = 2.0 * z1 + (fixed - 2.0 * rows3(rows3(z1, phis(), NN), (b_h[...], b_l[...]), NN))
    u1 = l1_ref[...] - z1
    send_chunks(1, l2 + u1)
    lo_ref[:, 0, :] = l2[:, 0:FEATS]
    l1_ref[...] = u1 + l2

    @pl.when(owner)
    def _():
        average(1)
        conclude(1)
        primal, dual = statistics(1)
        res[plane] = jnp.where(lane == 1, primal, jnp.where(lane == 3, dual, stats[...]))
        for peer in far_planes:
            for core in range(2):
                remote(res.at[plane], res.at[plane], send_res.at[0], recv_res.at[0], (in_plane(peer), core)).start()
        remote(res.at[plane], res.at[plane], send_res.at[0], recv_res.at[0], (slab, 0)).start()

    z2 = gathered(1)
    du_ref[:, 0, :] = (l1_ref[...] - z2)[:, 0:FEATS]
    co_ref[...] = z2[:, 0:FEATS]

    @pl.when(owner)
    def _():
        take(res.at[0:PLANE - 1], recv_res.at[0])

    @pl.when(jnp.logical_not(owner))
    def _():
        take(res, recv_res.at[0])

    total = functools.reduce(jnp.add, [res[i] for i in range(PLANE)])
    total = jnp.sqrt(total / (N_SLAB * R * FEATS))
    rh_ref[...] = jnp.concatenate([total[:, 0:2], total[:, 2:4]], 0)

    @pl.when(owner)
    def _():
        for k in range(2):
            take(outs.at[k, 0:PLANE - 1], send1.at[k])
            take(mids.at[k, 0:DEPTH - 1], send2.at[k])
            take(ins.at[k, 0:2 * PLANE - 1], send3.at[k])
        take(sent.at[0:2 * PLANE - 1], send_res.at[0])

    @pl.when(jnp.logical_not(owner))
    def _():
        for k in range(2):
            take(outs.at[k], send1.at[k])


def put_out(*refs):
    sems = refs[-1]
    copies = [pltpu.make_async_copy(refs[i], refs[4 + i], sems.at[i]) for i in range(4)]
    for copy in copies:
        copy.start()
    for copy in copies:
        copy.wait()


def shards(states, inputs, targets):
    vmem = pl.BlockSpec(memory_space=pltpu.VMEM)
    dma = pltpu.SemaphoreType.DMA
    f32 = lambda *shape: pltpu.VMEM(shape, F32)
    half = lambda *shape: pltpu.VMEM(shape, BF16)
    results = (
        jax.ShapeDtypeStruct((HALF, 1, FEATS), F32),
        jax.ShapeDtypeStruct((HALF, 1, FEATS), F32),
        jax.ShapeDtypeStruct((HALF, FEATS), F32),
        jax.ShapeDtypeStruct((2, 2), F32),
    )
    whole = pl.BlockSpec(memory_space=pl.ANY)
    operators, duals, consensus, history = pl.pallas_call(
        kernel,
        out_shape=results,
        in_specs=[vmem] * 3,
        out_specs=(vmem,) * 4,
        scratch_shapes=[
            f32(R, MINE), f32(1, MINE), f32(R, MINE),
            f32(WIDE, M), half(WIDE, M), half(WIDE, M), f32(M, M), f32(128, 128),
            half(M, WIDE), half(M, WIDE), f32(HALF, WIDE),
            f32(2, PLANE, 9, 128), f32(2, 2 * PLANE, 9, 128), f32(2, DEPTH, 19, 128),
            f32(2, PLANE, 9, 128), f32(2, 9, 128), f32(PLANE, 1, 128), f32(2 * PLANE, 1, 128), f32(1, 128),
            dma((6,)), dma((2,)), dma((2,)), dma((2,)), dma((2,)), dma((2,)), dma((2,)), dma((1,)), dma((1,)),
        ],
        compiler_params=pltpu.CompilerParams(
            collective_id=0, has_side_effects=True, vmem_limit_bytes=48 * 1024 * 1024
        ),
        name="consensus",
    )(states, inputs.reshape(1, MINE), targets)
    operators, duals, consensus, history = pl.pallas_call(
        put_out,
        out_shape=results,
        in_specs=[vmem] * 4,
        out_specs=(whole,) * 4,
        scratch_shapes=[dma((4,))],
        compiler_params=pltpu.CompilerParams(vmem_limit_bytes=1024 * 1024),
        name="put_out",
    )(operators, duals, consensus, history)
    return operators.transpose(1, 0, 2), duals.transpose(1, 0, 2), consensus, history


def solution(mesh):
    return jax.shard_map(
        shards,
        mesh=mesh,
        in_specs=(P(None, ("slab", "feat")), P(("slab", "feat")), P(None, ("slab", "feat"))),
        out_specs=(P("slab", "feat", None), P("slab", "feat", None), P("feat", None), P()),
        check_vma=False,
    )
```

```python
import functools

import jax
import jax.numpy as jnp
from jax import lax
from jax.experimental import pallas as pl
from jax.experimental.pallas import tpu as pltpu
from jax.sharding import PartitionSpec as P

F32, BF16 = jnp.float32, jnp.bfloat16
NN = (((1,), (0,)), ((), ()))
NT = (((1,), (1,)), ((), ()))
TN = (((0,), (0,)), ((), ()))
MESH = pl.DeviceIdType.MESH

R = 40
HALF = 20
FEATS = 862
WIDE = 896
PLANE = 16
DEPTH = 8
N_SLAB = 128
M = 512
MINE = 256
rho = 1.0


def dot(a, b, dims):
    return lax.dot_general(a, b, dims, preferred_element_type=F32)


def two(a):
    high = a.astype(BF16)
    return high, (a - high.astype(F32)).astype(BF16)


def dot3(a, b, dims):
    (ah, al), (bh, bl) = a, b
    return dot(ah, bh, dims) + (dot(ah, bl, dims) + dot(al, bh, dims))


def rows3(a, b, dims):
    rows, pad = a.shape[0], -a.shape[0] % 8
    if pad:
        a = jnp.concatenate([a, jnp.zeros((pad, a.shape[1]), F32)], 0)
    tall = rows + pad
    high = a.astype(BF16).astype(F32)
    both = jnp.concatenate([high, a - high], 0).astype(BF16)
    first = dot(both, b[0], dims)
    return (first[0:tall] + (first[tall:] + dot(high.astype(BF16), b[1], dims)))[0:rows]


def three(a):
    high = a.astype(BF16).astype(F32)
    rest = a - high
    mid = rest.astype(BF16).astype(F32)
    return high, mid, rest - mid


def stacks(x, u):
    def left_of(h, m, l):
        return [h, h, m, h, l, m]

    def right_of(h, m, l):
        return [h, m, h, l, h, m]

    xs, ss, us = three(x), three(x * x), three(u)
    halves = tuple(0.5 * s for s in ss)
    ends = [jnp.ones_like(u), jnp.zeros_like(u)]
    cat = lambda parts: jnp.concatenate(parts, 0).astype(BF16)
    return (
        cat(left_of(*xs)),
        cat(right_of(*xs)),
        cat(left_of(*halves) + left_of(*us) + ends),
        cat(right_of(*ss) + right_of(*us) + ends),
    )


def kernel_block(a, b):
    g = dot(a[0], b[1], TN)
    return g + dot(a[2], b[3], TN) + 0.5 * (g * g)


def add_diagonal(block):
    row = lax.broadcasted_iota(jnp.int32, block.shape, 0)
    col = lax.broadcasted_iota(jnp.int32, block.shape, 1)
    return block + jnp.where(row == col, rho * M, 0.0)


def invert(a, beside=(), n=128, w=16):
    beside = list(beside)
    tiles, wt = n // 8, w // 8
    lane = lax.broadcasted_iota(jnp.int32, (8, n), 1)
    sub = lax.broadcasted_iota(jnp.int32, (8, n), 0)

    def row_of(x, i):
        return jnp.broadcast_to(x[i:i + 1, :], (8, n))

    a = [a[8 * t:8 * t + 8] for t in range(tiles)]
    for j in range(n // w):
        k0, t0 = w * j, wt * j
        near = [t % tiles for t in range(t0 + wt, t0 + 2 * wt)] if j + 1 < n // w else []
        rest = [t for t in range(tiles) if t not in near and not t0 <= t < t0 + wt]
        inside = (lane >= k0) & (lane < k0 + w)

        def spread(t, k):
            return jnp.broadcast_to(a[t][:, k0 + k:k0 + k + 1], (8, n))

        col = [[spread(t0 + s, k) + 0.0 for s in range(wt)] for k in range(w)]
        ahead = {(t, k): spread(t, k) for k in range(w) for t in near}
        row = [jnp.where(inside, (lane == k0 + 8 * s + sub).astype(F32), a[t0 + s]) for s in range(wt)]
        scale = [None] * wt
        for k in range(w):
            if k == 4 and beside:
                beside.pop(0)()
            s0, i = divmod(k, 8)
            inv = 1.0 / row_of(col[k][s0], i)
            scale[s0] = inv if i == 0 else jnp.where(sub == i, inv, scale[s0])
            off = list(col[k])
            off[s0] = jnp.where(sub == i, 0.0, off[s0])
            for m in range(k + 1, w):
                factor = row_of(col[m][s0], i)
                if m == k + 1:
                    col[m] = [c - (o * factor) * inv for c, o in zip(col[m], off)]
                else:
                    factor = factor * inv
                    col[m] = [c - o * factor for c, o in zip(col[m], off)]
            factor = row_of(row[s0], i) * inv
            row = [r - o * factor for r, o in zip(row, off)]
        row = [r * s for r, s in zip(row, scale)]
        pivots = [row_of(row[k // 8], k % 8) for k in range(w)] if near else []
        for t in near:
            terms = [ahead[t, k] * pivots[k] for k in range(w)]
            while len(terms) > 1:
                terms = [functools.reduce(jnp.add, terms[i:i + 2]) for i in range(0, len(terms), 2)]
            a[t] = jnp.where(inside, 0.0, a[t]) - terms[0]
        old = jnp.concatenate([a[t] for t in rest], 0)
        old_h, old_l = two(old)
        new_h, new_l = two(jnp.concatenate(row, 0))
        gap = [jnp.zeros((m, n), BF16) for m in (k0, n - k0 - w)]

        def padded(x):
            return jnp.concatenate([p for p in (gap[0], x, gap[1]) if p.shape[0]], 0)

        high, low = padded(new_h), padded(new_l)
        change = dot(jnp.concatenate([old_h, old_l], 1), jnp.concatenate([high, high], 0), NN) + dot(old_h, low, NN)
        for i, t in enumerate(rest):
            a[t] = jnp.where(inside, 0.0, a[t]) - change[8 * i:8 * i + 8]
        for s in range(wt):
            a[t0 + s] = row[s]
    for work in beside:
        work()
    return jnp.concatenate(a, 0)


def write_features(phi_ref, x_ref, u, at):
    cols = pl.ds(at, MINE)
    phi_ref[0:R, cols] = x_ref[...]
    off = R
    for i in range(R):
        phi_ref[off:off + R - i, cols] = x_ref[i:i + 1, :] * x_ref[i:R, :]
        off += R - i
    phi_ref[off:off + 1, cols] = u
    phi_ref[off + 1:off + 2, cols] = jnp.ones_like(u)
    phi_ref[off + 2:WIDE, cols] = jnp.zeros((WIDE - FEATS, MINE), F32)


def to_chunks(whole, out_ref):
    def piece(r, n, c):
        return whole[r:r + n, 128 * c:128 * c + 128]

    for c in range(7):
        out_ref[2 * c, 0:8, :] = piece(0, 8, c)
        out_ref[2 * c + 1, 0:8, :] = piece(8, 8, c)
    out_ref[14, 0:8, :] = jnp.concatenate([piece(16, 4, 0), piece(16, 4, 1)], 0)
    out_ref[15, 0:8, :] = jnp.concatenate([piece(16, 4, 2), piece(16, 4, 3)], 0)
    for i in range(12):
        out_ref[i, 8:9, :] = piece(16 + i % 4, 1, 4 + i // 4)
    for i in range(12, 16):
        out_ref[i, 8:9, :] = jnp.zeros((1, 128), F32)


def from_chunks(ref):
    columns = []
    for c in range(7):
        if c < 4:
            last = ref[14 + c // 2, 4 * (c % 2):4 * (c % 2) + 4, :]
        else:
            last = jnp.concatenate([ref[4 * (c - 4) + i, 8:9, :] for i in range(4)], 0)
        columns.append(jnp.concatenate([ref[2 * c, 0:8, :], ref[2 * c + 1, 0:8, :], last], 0))
    return jnp.concatenate(columns, 1)


def rows_sum(main, ext):
    return jnp.sum(main, 0, keepdims=True) + ext


def kernel(
    near_ref, lo_ref, du_ref, co_ref, rh_ref,
    far_ref, phi, phi_h, phi_l, s_ref, d_ref, p_ref, b_h, b_l, l1_ref,
    outs, ins, mids, zs, zs_far, res, sent, stats,
    pair_sems, send1, recv1, send2, recv2, send3, recv3, send_res, recv_res,
):
    (x_ref, t_ref, u_ref), (xo, to, uo) = (
        [ref.at[0:R], ref.at[R:2 * R], ref.at[2 * R:2 * R + 1]] for ref in (near_ref, far_ref)
    )
    slab = lax.axis_index("slab")
    feat = lax.axis_index("feat")
    plane = lax.rem(slab, PLANE)
    depth = lax.div(slab, PLANE)
    line, spot = lax.div(plane, 4), lax.rem(plane, 4)
    other = 1 - feat
    owner = feat == 1
    steps = sorted(((dy, dx) for dy in range(4) for dx in range(4) if dy or dx), key=lambda d: -sum(min(v, 4 - v) for v in d))
    far_planes = [4 * lax.rem(line + dy, 4) + lax.rem(spot + dx, 4) for dy, dx in steps]
    far_depths = [lax.rem(depth + d, DEPTH) for d in (4, 3, 5, 2, 6, 1, 7)]

    def in_plane(i):
        return depth * PLANE + i

    def in_depth(i):
        return i * PLANE + plane

    barrier = pltpu.get_barrier_semaphore()

    def greet(s, f):
        pl.semaphore_signal(barrier, inc=1, device_id=(s, f), device_id_type=MESH)

    greet(slab, other)
    for peer in far_planes:
        greet(in_plane(peer), 1)

    @pl.when(owner)
    def _():
        for peer in far_planes:
            greet(in_plane(peer), 0)
        for peer in far_depths:
            greet(in_depth(peer), 1)

    u_own = u_ref[...]
    own = stacks(x_ref[...], u_own)
    s_ref[0:MINE, 0:MINE] = add_diagonal(kernel_block(own, own))
    write_features(phi, x_ref, u_own, 0)

    pl.semaphore_wait(barrier, PLANE + feat * (PLANE + DEPTH - 2))
    pair = pltpu.make_async_remote_copy(
        src_ref=near_ref, dst_ref=far_ref, send_sem=pair_sems.at[0], recv_sem=pair_sems.at[1],
        device_id=(slab, other), device_id_type=MESH,
    )
    pair.start()

    def block(r, c):
        return s_ref[128 * r:128 * r + 128, 128 * c:128 * c + 128]

    def next_block(kb, inverse):
        ahead = dot3(inverse, two(block(kb, kb + 1)), NN)
        return block(kb + 1, kb + 1) - dot3(two(block(kb + 1, kb)), two(ahead), NN)

    def eliminate(kb, inverse):
        rows = slice(128 * kb, 128 * kb + 128)

        def pivots():
            high = two(inverse)
            p_ref[kb % 2] = jnp.concatenate(
                [inverse if c == kb else dot3(high, two(block(kb, c)), NN) for c in range(4)], 1
            )

        def update(rb):
            change = dot3(two(block(rb, kb)), two(p_ref[kb % 2]), NN)
            s_ref[128 * rb:128 * rb + 128, rows] = jnp.zeros((128, 128), F32)
            s_ref[128 * rb:128 * rb + 128, :] -= change

        def close():
            s_ref[rows, :] = p_ref[kb % 2]

        order = [(kb + i) % 4 for i in range(1, 4)]
        return [pivots] + [functools.partial(update, rb) for rb in order] + [close]

    def far_blocks():
        u_far = uo[...]
        own = stacks(x_ref[...], u_ref[...])
        far = stacks(xo[...], u_far)
        s_ref[0:MINE, MINE:M] = kernel_block(own, far)
        s_ref[MINE:M, 0:MINE] = kernel_block(far, own)
        s_ref[MINE:M, MINE:M] = add_diagonal(kernel_block(far, far))

    def split_features(i):
        part = slice(224 * i, 224 * i + 224)
        phi_h[part], phi_l[part] = two(phi[part])

    inverse = invert(block(0, 0))
    pivot = next_block(0, two(inverse))
    pair.wait()
    inverse = invert(pivot, [far_blocks] + eliminate(0, inverse) + [lambda: write_features(phi, xo, uo[...], MINE)])
    pivot = next_block(1, two(inverse))
    inverse = invert(pivot, eliminate(1, inverse) + [functools.partial(split_features, i) for i in range(4)])
    pivot = next_block(2, two(inverse))

    def phis():
        return phi_h[...], phi_l[...]

    first = feat == 0
    rest_rows = slice(0, 384)
    kept = {}

    def solve_rest():
        targets = jnp.concatenate(
            [jnp.where(first, t[0:HALF, :], t[HALF:R, :]) for t in (t_ref, to)], 1
        )
        left = rows3(targets[:, rest_rows], two(s_ref[rest_rows, :]), NN)
        kept["v"] = targets[:, 384:M] - left[:, 384:M]
        kept["y"] = jnp.concatenate([left[:, rest_rows], jnp.zeros((HALF, 128), F32)], 1)

    def apply_rest():
        kept["ly"] = rows3(kept["y"], phis(), NT)

    def last_features():
        kept["last"] = two(s_ref[384:M, rest_rows])
        kept["g3"] = two(
            dot3(kept["last"], (phi_h[:, rest_rows], phi_l[:, rest_rows]), NT) + phi[:, 384:M].T
        )

    inverse = invert(pivot, eliminate(2, inverse) + [solve_rest, apply_rest, last_features])
    v, y, ly, last, g3 = (kept[name] for name in ("v", "y", "ly", "last", "g3"))
    vd = rows3(v, two(inverse), NN)
    l1 = ly + rows3(vd, g3, NN)
    l1_ref[...] = l1
    d_ref[...] = inverse

    def remote(src, dst, send, recv, device):
        return pltpu.make_async_remote_copy(
            src_ref=src, dst_ref=dst, send_sem=send, recv_sem=recv, device_id=device, device_id_type=MESH
        )

    def take(ref, sem):
        pltpu.make_async_copy(ref, ref, sem).wait()

    def send_chunks(k, whole):
        to_chunks(whole, outs.at[k])

        def scatter(peer):
            remote(
                outs.at[k, peer], ins.at[k, feat * PLANE + plane], send1.at[k], recv1.at[k], (in_plane(peer), 1)
            ).start()

        for peer in far_planes:
            scatter(peer)

        @pl.when(owner)
        def _():
            ins[k, PLANE + plane] = outs[k, plane]

        @pl.when(jnp.logical_not(owner))
        def _():
            scatter(plane)

    def parts(ref, *at):
        return [ref[(*at, slice(0, 8))], ref[(*at, slice(8, 9))]]

    def add_up(pieces):
        return [functools.reduce(jnp.add, [p[i] for p in pieces]) for i in range(2)]

    def squares(pieces, mean):
        total = [jnp.zeros((8, 128), F32), jnp.zeros((1, 128), F32)]
        for piece in pieces:
            for i in range(2):
                gap = piece[i] - mean[i]
                total[i] = total[i] + gap * gap
        return jnp.sum(total[0], 0, keepdims=True) + total[1]

    def consensus_of(k, half):
        return parts(zs, k, plane) if half else parts(zs_far, k)

    def layer(k, z, half):
        return [mids[k, z, 8 * half:8 * half + 8, :], mids[k, z, 16 + half:17 + half, :]]

    def average(k):
        take(ins.at[k, 0:2 * PLANE - 1], recv1.at[k])
        spread = jnp.zeros((1, 128), F32)
        for half in range(2):
            sent = [parts(ins, k, PLANE * half + s) for s in range(PLANE)]
            total = mean = add_up(sent)
            operators = sent
            if k == 1:
                last = consensus_of(0, half)
                before = [parts(ins, 0, PLANE * half + s) for s in range(PLANE)]
                operators = [[p - (b - z) for p, b, z in zip(new, old, last)] for new, old in zip(sent, before)]
                mean = add_up(operators)
            mids[k, depth, 8 * half:8 * half + 8, :] = total[0]
            mids[k, depth, 16 + half:17 + half, :] = total[1]
            spread = spread + squares(operators, [m / PLANE for m in mean])
        mids[k, depth, 18:19, :] = spread
        for peer in far_depths:
            remote(
                mids.at[k, depth], mids.at[k, depth], send2.at[k], recv2.at[k], (in_depth(peer), 1)
            ).start()

    def conclude(k):
        take(mids.at[k, 0:DEPTH - 1], recv2.at[k])
        means = []
        for half in range(2):
            means.append([m / N_SLAB for m in add_up([layer(k, z, half) for z in range(DEPTH)])])
        zs_far[k, 0:8, :] = means[0][0]
        zs_far[k, 8:9, :] = means[0][1]
        zs[k, plane, 0:8, :] = means[1][0]
        zs[k, plane, 8:9, :] = means[1][1]

        def gather(src, peer, core):
            remote(src, zs.at[k, plane], send3.at[k], recv3.at[k], (in_plane(peer), core)).start()

        for peer in far_planes:
            gather(zs_far.at[k], peer, 0)
            gather(zs.at[k, plane], peer, 1)
        gather(zs_far.at[k], plane, 0)

    def statistics(k):
        primal = jnp.zeros((1, 128), F32)
        dual = jnp.zeros((1, 128), F32)
        for half in range(2):
            mean = consensus_of(k, half)
            layers = [layer(k, z, half) for z in range(DEPTH)]
            if k == 0:
                last = [jnp.zeros((8, 128), F32), jnp.zeros((1, 128), F32)]
            else:
                last = consensus_of(0, half)
                before = [layer(0, z, half) for z in range(DEPTH)]
                layers = [[p - (b - PLANE * z) for p, b, z in zip(new, old, last)] for new, old in zip(layers, before)]
            primal = primal + PLANE * squares([[p / PLANE for p in each] for each in layers], mean)
            dual = dual + squares([mean], last)
        for z in range(DEPTH):
            primal = primal + mids[k, z, 18:19, :]
        return jnp.sum(primal, 1, keepdims=True), N_SLAB * rho * rho * jnp.sum(dual, 1, keepdims=True)

    def gathered(k):
        @pl.when(owner)
        def _():
            take(zs.at[k, 0:PLANE - 1], recv3.at[k])

        @pl.when(jnp.logical_not(owner))
        def _():
            take(zs.at[k], recv3.at[k])

        return from_chunks(zs.at[k])

    lane = lax.broadcasted_iota(jnp.int32, (1, 128), 1)

    send_chunks(0, l1)
    w1 = y + jnp.concatenate([rows3(vd, last, NN), vd], 1)
    for work in eliminate(3, d_ref[...]):
        work()
    inverse = two(s_ref[...])
    fixed = rows3(w1 - rho * M * rows3(w1, inverse, NN), phis(), NT)

    @pl.when(owner)
    def _():
        average(0)

    high, low = two(dot3(inverse, (phi_h[...], phi_l[...]), NT))
    b_h[...] = high
    b_l[...] = low

    @pl.when(owner)
    def _():
        conclude(0)
        primal, dual = statistics(0)
        stats[...] = jnp.where(lane == 0, primal, jnp.where(lane == 2, dual, 0.0))

    z1 = gathered(0)
    l2 = 2.0 * z1 + (fixed - 2.0 * rows3(rows3(z1, phis(), NN), (b_h[...], b_l[...]), NN))
    u1 = l1_ref[...] - z1
    send_chunks(1, l2 + u1)
    lo_ref[:, 0, :] = l2[:, 0:FEATS]
    l1_ref[...] = u1 + l2

    @pl.when(owner)
    def _():
        average(1)
        conclude(1)
        primal, dual = statistics(1)
        res[plane] = jnp.where(lane == 1, primal, jnp.where(lane == 3, dual, stats[...]))
        for peer in far_planes:
            for core in range(2):
                remote(res.at[plane], res.at[plane], send_res.at[0], recv_res.at[0], (in_plane(peer), core)).start()
        remote(res.at[plane], res.at[plane], send_res.at[0], recv_res.at[0], (slab, 0)).start()

    z2 = gathered(1)
    du_ref[:, 0, :] = (l1_ref[...] - z2)[:, 0:FEATS]
    co_ref[...] = z2[:, 0:FEATS]

    @pl.when(owner)
    def _():
        take(res.at[0:PLANE - 1], recv_res.at[0])

    @pl.when(jnp.logical_not(owner))
    def _():
        take(res, recv_res.at[0])

    total = functools.reduce(jnp.add, [res[i] for i in range(PLANE)])
    total = jnp.sqrt(total / (N_SLAB * R * FEATS))
    rh_ref[...] = jnp.concatenate([total[:, 0:2], total[:, 2:4]], 0)

    @pl.when(owner)
    def _():
        for k in range(2):
            take(outs.at[k, 0:PLANE - 1], send1.at[k])
            take(mids.at[k, 0:DEPTH - 1], send2.at[k])
            take(ins.at[k, 0:2 * PLANE - 1], send3.at[k])
        take(sent.at[0:2 * PLANE - 1], send_res.at[0])

    @pl.when(jnp.logical_not(owner))
    def _():
        for k in range(2):
            take(outs.at[k], send1.at[k])


def put_out(*refs):
    sems = refs[-1]
    copies = [pltpu.make_async_copy(refs[i], refs[4 + i], sems.at[i]) for i in range(4)]
    for copy in copies:
        copy.start()
    for copy in copies:
        copy.wait()


def shards(states, inputs, targets):
    vmem = pl.BlockSpec(memory_space=pltpu.VMEM)
    dma = pltpu.SemaphoreType.DMA
    f32 = lambda *shape: pltpu.VMEM(shape, F32)
    half = lambda *shape: pltpu.VMEM(shape, BF16)
    results = (
        jax.ShapeDtypeStruct((HALF, 1, FEATS), F32),
        jax.ShapeDtypeStruct((HALF, 1, FEATS), F32),
        jax.ShapeDtypeStruct((HALF, FEATS), F32),
        jax.ShapeDtypeStruct((2, 2), F32),
    )
    whole = pl.BlockSpec(memory_space=pl.ANY)
    packed = jnp.concatenate([states, targets, jnp.broadcast_to(inputs[None], (8, MINE))], 0)
    operators, duals, consensus, history = pl.pallas_call(
        kernel,
        out_shape=results,
        in_specs=[vmem],
        out_specs=(vmem,) * 4,
        scratch_shapes=[
            f32(2 * R + 8, MINE),
            f32(WIDE, M), half(WIDE, M), half(WIDE, M), f32(M, M), f32(128, 128), f32(2, 128, M),
            half(M, WIDE), half(M, WIDE), f32(HALF, WIDE),
            f32(2, PLANE, 9, 128), f32(2, 2 * PLANE, 9, 128), f32(2, DEPTH, 19, 128),
            f32(2, PLANE, 9, 128), f32(2, 9, 128), f32(PLANE, 1, 128), f32(2 * PLANE, 1, 128), f32(1, 128),
            dma((2,)), dma((2,)), dma((2,)), dma((2,)), dma((2,)), dma((2,)), dma((2,)), dma((1,)), dma((1,)),
        ],
        compiler_params=pltpu.CompilerParams(
            collective_id=0, has_side_effects=True, vmem_limit_bytes=48 * 1024 * 1024
        ),
        name="consensus",
    )(packed)
    operators, duals, consensus, history = pl.pallas_call(
        put_out,
        out_shape=results,
        in_specs=[vmem] * 4,
        out_specs=(whole,) * 4,
        scratch_shapes=[dma((4,))],
        compiler_params=pltpu.CompilerParams(vmem_limit_bytes=1024 * 1024),
        name="put_out",
    )(operators, duals, consensus, history)
    return operators.transpose(1, 0, 2), duals.transpose(1, 0, 2), consensus, history


def solution(mesh):
    return jax.shard_map(
        shards,
        mesh=mesh,
        in_specs=(P(None, ("slab", "feat")), P(("slab", "feat")), P(None, ("slab", "feat"))),
        out_specs=(P("slab", "feat", None), P("slab", "feat", None), P("feat", None), P()),
        check_vma=False,
    )
```

```python
import functools

import jax
import jax.numpy as jnp
from jax import lax
from jax.experimental import pallas as pl
from jax.experimental.pallas import tpu as pltpu
from jax.sharding import PartitionSpec as P

F32, BF16 = jnp.float32, jnp.bfloat16
NN = (((1,), (0,)), ((), ()))
NT = (((1,), (1,)), ((), ()))
TN = (((0,), (0,)), ((), ()))
MESH = pl.DeviceIdType.MESH

R = 40
HALF = 20
FEATS = 862
WIDE = 896
PLANE = 16
DEPTH = 8
N_SLAB = 128
M = 512
MINE = 256
rho = 1.0


def dot(a, b, dims):
    return lax.dot_general(a, b, dims, preferred_element_type=F32)


def two(a):
    high = a.astype(BF16)
    return high, (a - high.astype(F32)).astype(BF16)


def dot3(a, b, dims):
    (ah, al), (bh, bl) = a, b
    return dot(ah, bh, dims) + (dot(ah, bl, dims) + dot(al, bh, dims))


def left3(a):
    high, low = two(a)
    return jnp.concatenate([high, low, high], 1)


def right3(b):
    high, low = two(b)
    return jnp.concatenate([high, high, low], 0)


def rows3(a, b, dims):
    rows, pad = a.shape[0], -a.shape[0] % 8
    if pad:
        a = jnp.concatenate([a, jnp.zeros((pad, a.shape[1]), F32)], 0)
    tall = rows + pad
    high = a.astype(BF16).astype(F32)
    both = jnp.concatenate([high, a - high], 0).astype(BF16)
    first = dot(both, b[0], dims)
    return (first[0:tall] + (first[tall:] + dot(high.astype(BF16), b[1], dims)))[0:rows]


def three(a):
    high = a.astype(BF16).astype(F32)
    rest = a - high
    mid = rest.astype(BF16).astype(F32)
    return high, mid, rest - mid


def stacks(x, u):
    def left_of(h, m, l):
        return [h, h, m, h, l, m]

    def right_of(h, m, l):
        return [h, m, h, l, h, m]

    xs, ss, us = three(x), three(x * x), three(u)
    halves = tuple(0.5 * s for s in ss)
    ends = [jnp.ones_like(u), jnp.zeros_like(u)]
    cat = lambda parts: jnp.concatenate(parts, 0).astype(BF16)
    return (
        cat(left_of(*xs)),
        cat(right_of(*xs)),
        cat(left_of(*halves) + left_of(*us) + ends),
        cat(right_of(*ss) + right_of(*us) + ends),
    )


def kernel_block(a, b):
    g = dot(a[0], b[1], TN)
    return g + dot(a[2], b[3], TN) + 0.5 * (g * g)


def add_diagonal(block):
    row = lax.broadcasted_iota(jnp.int32, block.shape, 0)
    col = lax.broadcasted_iota(jnp.int32, block.shape, 1)
    return block + jnp.where(row == col, rho * M, 0.0)


def invert(a, beside=(), n=128, w=16):
    beside = list(beside)
    tiles, wt = n // 8, w // 8
    lane = lax.broadcasted_iota(jnp.int32, (8, n), 1)
    sub = lax.broadcasted_iota(jnp.int32, (8, n), 0)

    def row_of(x, i):
        return jnp.broadcast_to(x[i:i + 1, :], (8, n))

    a = [a[8 * t:8 * t + 8] for t in range(tiles)]
    for j in range(n // w):
        k0, t0 = w * j, wt * j
        near = [t % tiles for t in range(t0 + wt, t0 + 2 * wt)] if j + 1 < n // w else []
        rest = [t for t in range(tiles) if t not in near and not t0 <= t < t0 + wt]
        inside = (lane >= k0) & (lane < k0 + w)

        def spread(t, k):
            return jnp.broadcast_to(a[t][:, k0 + k:k0 + k + 1], (8, n))

        col = [[spread(t0 + s, k) + 0.0 for s in range(wt)] for k in range(w)]
        ahead = {(t, k): spread(t, k) for k in range(w) for t in near}
        row = [jnp.where(inside, (lane == k0 + 8 * s + sub).astype(F32), a[t0 + s]) for s in range(wt)]
        scale = [None] * wt
        for k in range(w):
            if k == 4 and beside:
                beside.pop(0)()
            s0, i = divmod(k, 8)
            inv = 1.0 / row_of(col[k][s0], i)
            scale[s0] = inv if i == 0 else jnp.where(sub == i, inv, scale[s0])
            off = list(col[k])
            off[s0] = jnp.where(sub == i, 0.0, off[s0])
            for m in range(k + 1, w):
                factor = row_of(col[m][s0], i)
                if m == k + 1:
                    col[m] = [c - (o * factor) * inv for c, o in zip(col[m], off)]
                else:
                    factor = factor * inv
                    col[m] = [c - o * factor for c, o in zip(col[m], off)]
            factor = row_of(row[s0], i) * inv
            row = [r - o * factor for r, o in zip(row, off)]
        row = [r * s for r, s in zip(row, scale)]
        pivots = [row_of(row[k // 8], k % 8) for k in range(w)] if near else []
        for t in near:
            terms = [ahead[t, k] * pivots[k] for k in range(w)]
            while len(terms) > 1:
                terms = [functools.reduce(jnp.add, terms[i:i + 2]) for i in range(0, len(terms), 2)]
            a[t] = jnp.where(inside, 0.0, a[t]) - terms[0]
        old = jnp.concatenate([a[t] for t in rest], 0)
        old_h, old_l = two(old)
        new_h, new_l = two(jnp.concatenate(row, 0))
        gap = [jnp.zeros((m, n), BF16) for m in (k0, n - k0 - w)]

        def padded(x):
            return jnp.concatenate([p for p in (gap[0], x, gap[1]) if p.shape[0]], 0)

        high, low = padded(new_h), padded(new_l)
        change = dot(jnp.concatenate([old_h, old_l, old_h], 1), jnp.concatenate([high, high, low], 0), NN)
        for i, t in enumerate(rest):
            a[t] = jnp.where(inside, 0.0, a[t]) - change[8 * i:8 * i + 8]
        for s in range(wt):
            a[t0 + s] = row[s]
    for work in beside:
        work()
    return jnp.concatenate(a, 0)


def write_features(phi_ref, x_ref, u, at):
    cols = pl.ds(at, MINE)
    phi_ref[0:R, cols] = x_ref[...]
    off = R
    for i in range(R):
        phi_ref[off:off + R - i, cols] = x_ref[i:i + 1, :] * x_ref[i:R, :]
        off += R - i
    phi_ref[off:off + 1, cols] = u
    phi_ref[off + 1:off + 2, cols] = jnp.ones_like(u)
    phi_ref[off + 2:WIDE, cols] = jnp.zeros((WIDE - FEATS, MINE), F32)


def to_chunks(whole, out_ref):
    def piece(r, n, c):
        return whole[r:r + n, 128 * c:128 * c + 128]

    for c in range(7):
        out_ref[2 * c, 0:8, :] = piece(0, 8, c)
        out_ref[2 * c + 1, 0:8, :] = piece(8, 8, c)
    out_ref[14, 0:8, :] = jnp.concatenate([piece(16, 4, 0), piece(16, 4, 1)], 0)
    out_ref[15, 0:8, :] = jnp.concatenate([piece(16, 4, 2), piece(16, 4, 3)], 0)
    for i in range(12):
        out_ref[i, 8:9, :] = piece(16 + i % 4, 1, 4 + i // 4)
    for i in range(12, 16):
        out_ref[i, 8:9, :] = jnp.zeros((1, 128), F32)


def from_chunks(ref):
    columns = []
    for c in range(7):
        if c < 4:
            last = ref[14 + c // 2, 4 * (c % 2):4 * (c % 2) + 4, :]
        else:
            last = jnp.concatenate([ref[4 * (c - 4) + i, 8:9, :] for i in range(4)], 0)
        columns.append(jnp.concatenate([ref[2 * c, 0:8, :], ref[2 * c + 1, 0:8, :], last], 0))
    return jnp.concatenate(columns, 1)


def rows_sum(main, ext):
    return jnp.sum(main, 0, keepdims=True) + ext


def kernel(
    near_ref, u_ref, lo_ref, du_ref, co_ref, rh_ref,
    far_ref, uo, phi, phi_h, phi_l, s_ref, d_ref, p_ref, b_h, b_l, l1_ref,
    outs, ins, mids, sqs, zs, zs_far, res, sent, stats,
    pair_sems, send1, recv1, send2, recv2, send3, recv3, send_sq, recv_sq, send_res, recv_res,
):
    (x_ref, t_ref), (xo, to) = ([ref.at[0:R], ref.at[R:2 * R]] for ref in (near_ref, far_ref))
    slab = lax.axis_index("slab")
    feat = lax.axis_index("feat")
    plane = lax.rem(slab, PLANE)
    depth = lax.div(slab, PLANE)
    line, spot = lax.div(plane, 4), lax.rem(plane, 4)
    other = 1 - feat
    owner = feat == 1
    steps = sorted(((dy, dx) for dy in range(4) for dx in range(4) if dy or dx), key=lambda d: -sum(min(v, 4 - v) for v in d))
    far_planes = [4 * lax.rem(line + dy, 4) + lax.rem(spot + dx, 4) for dy, dx in steps]
    far_depths = [lax.rem(depth + d, DEPTH) for d in (4, 3, 5, 2, 6, 1, 7)]

    def in_plane(i):
        return depth * PLANE + i

    def in_depth(i):
        return i * PLANE + plane

    barrier = pltpu.get_barrier_semaphore()

    def greet(s, f):
        pl.semaphore_signal(barrier, inc=1, device_id=(s, f), device_id_type=MESH)

    greet(slab, other)
    for peer in far_planes:
        greet(in_plane(peer), 1)

    @pl.when(owner)
    def _():
        for peer in far_planes:
            greet(in_plane(peer), 0)
        for peer in far_depths:
            greet(in_depth(peer), 1)

    u_own = u_ref[...]
    own = stacks(x_ref[...], u_own)
    s_ref[0:MINE, 0:MINE] = add_diagonal(kernel_block(own, own))

    pl.semaphore_wait(barrier, PLANE + feat * (PLANE + DEPTH - 2))
    pair = [
        pltpu.make_async_remote_copy(
            src_ref=src, dst_ref=dst, send_sem=pair_sems.at[i], recv_sem=pair_sems.at[2 + i],
            device_id=(slab, other), device_id_type=MESH,
        )
        for i, (src, dst) in enumerate(((near_ref, far_ref), (u_ref, uo)))
    ]
    for copy in pair:
        copy.start()

    def block(r, c):
        return s_ref[128 * r:128 * r + 128, 128 * c:128 * c + 128]

    def next_block(kb, inverse):
        ahead = dot(left3(inverse), right3(block(kb, kb + 1)), NN)
        return block(kb + 1, kb + 1) - dot(left3(block(kb + 1, kb)), right3(ahead), NN)

    def eliminate(kb, inverse):
        rows = slice(128 * kb, 128 * kb + 128)

        def pivots():
            left = left3(inverse)
            new = jnp.concatenate(
                [inverse if c == kb else dot(left, right3(block(kb, c)), NN) for c in range(4)], 1
            )
            s_ref[rows, :] = new
            p_ref[kb % 2] = right3(new)

        def update(rb):
            at = slice(128 * rb, 128 * rb + 128)
            change = dot(left3(block(rb, kb)), p_ref[kb % 2], NN)
            for c in range(4):
                old = 0.0 if c == kb else block(rb, c)
                s_ref[at, 128 * c:128 * c + 128] = old - change[:, 128 * c:128 * c + 128]

        return [pivots] + [functools.partial(update, (kb + i) % 4) for i in range(1, 4)]

    def far_blocks():
        u_far = uo[...]
        own = stacks(x_ref[...], u_ref[...])
        far = stacks(xo[...], u_far)
        s_ref[0:MINE, MINE:M] = kernel_block(own, far)
        s_ref[MINE:M, 0:MINE] = kernel_block(far, own)
        s_ref[MINE:M, MINE:M] = add_diagonal(kernel_block(far, far))

    def split_features(i):
        part = slice(224 * i, 224 * i + 224)
        phi_h[part], phi_l[part] = two(phi[part])

    inverse = invert(block(0, 0), [lambda: write_features(phi, x_ref, u_ref[...], 0)])
    pivot = next_block(0, inverse)
    for copy in pair:
        copy.wait()
    inverse = invert(pivot, [far_blocks] + eliminate(0, inverse) + [lambda: write_features(phi, xo, uo[...], MINE)])
    pivot = next_block(1, inverse)
    inverse = invert(pivot, eliminate(1, inverse) + [functools.partial(split_features, i) for i in range(4)])
    pivot = next_block(2, inverse)

    def phis():
        return phi_h[...], phi_l[...]

    first = feat == 0
    rest_rows = slice(0, 384)
    kept = {}

    def solve_rest():
        targets = jnp.concatenate(
            [jnp.where(first, t[0:HALF, :], t[HALF:R, :]) for t in (t_ref, to)], 1
        )
        left = rows3(targets[:, rest_rows], two(s_ref[rest_rows, :]), NN)
        kept["v"] = targets[:, 384:M] - left[:, 384:M]
        kept["y"] = jnp.concatenate([left[:, rest_rows], jnp.zeros((HALF, 128), F32)], 1)

    def apply_rest():
        kept["ly"] = rows3(kept["y"], phis(), NT)

    def last_features():
        kept["last"] = two(s_ref[384:M, rest_rows])
        kept["g3"] = two(
            dot3(kept["last"], (phi_h[:, rest_rows], phi_l[:, rest_rows]), NT) + phi[:, 384:M].T
        )

    inverse = invert(pivot, eliminate(2, inverse) + [solve_rest, apply_rest, last_features])
    v, y, ly, last, g3 = (kept[name] for name in ("v", "y", "ly", "last", "g3"))
    vd = rows3(v, two(inverse), NN)
    l1 = ly + rows3(vd, g3, NN)
    l1_ref[...] = l1
    d_ref[...] = inverse

    def remote(src, dst, send, recv, device):
        return pltpu.make_async_remote_copy(
            src_ref=src, dst_ref=dst, send_sem=send, recv_sem=recv, device_id=device, device_id_type=MESH
        )

    def take(ref, sem):
        pltpu.make_async_copy(ref, ref, sem).wait()

    def send_chunks(k, whole):
        to_chunks(whole, outs.at[k])

        def scatter(peer):
            remote(
                outs.at[k, peer], ins.at[k, feat * PLANE + plane], send1.at[k], recv1.at[k], (in_plane(peer), 1)
            ).start()

        for peer in far_planes:
            scatter(peer)

        @pl.when(owner)
        def _():
            ins[k, PLANE + plane] = outs[k, plane]

        @pl.when(jnp.logical_not(owner))
        def _():
            scatter(plane)

    def parts(ref, *at):
        return [ref[(*at, slice(0, 8))], ref[(*at, slice(8, 9))]]

    def add_up(pieces):
        return [functools.reduce(jnp.add, [p[i] for p in pieces]) for i in range(2)]

    def squares(pieces, mean):
        total = [jnp.zeros((8, 128), F32), jnp.zeros((1, 128), F32)]
        for piece in pieces:
            for i in range(2):
                gap = piece[i] - mean[i]
                total[i] = total[i] + gap * gap
        return jnp.sum(total[0], 0, keepdims=True) + total[1]

    def consensus_of(k, half):
        return parts(zs, k, plane) if half else parts(zs_far, k)

    def layer(k, z, half):
        return [mids[k, z, 8 * half:8 * half + 8, :], mids[k, z, 16 + half:17 + half, :]]

    def average(k):
        take(ins.at[k, 0:2 * PLANE - 1], recv1.at[k])
        totals = [add_up([parts(ins, k, PLANE * half + s) for s in range(PLANE)]) for half in range(2)]
        for half in range(2):
            mids[k, depth, 8 * half:8 * half + 8, :] = totals[half][0]
            mids[k, depth, 16 + half:17 + half, :] = totals[half][1]
        for peer in far_depths:
            remote(
                mids.at[k, depth], mids.at[k, depth], send2.at[k], recv2.at[k], (in_depth(peer), 1)
            ).start()
        spread = jnp.zeros((1, 128), F32)
        for half in range(2):
            mean = totals[half]
            operators = [parts(ins, k, PLANE * half + s) for s in range(PLANE)]
            if k == 1:
                last = consensus_of(0, half)
                before = [parts(ins, 0, PLANE * half + s) for s in range(PLANE)]
                operators = [[p - (b - z) for p, b, z in zip(new, old, last)] for new, old in zip(operators, before)]
                mean = add_up(operators)
            spread = spread + squares(operators, [m / PLANE for m in mean])
        sqs[k, depth] = spread
        for peer in far_depths:
            remote(
                sqs.at[k, depth], sqs.at[k, depth], send_sq.at[k], recv_sq.at[k], (in_depth(peer), 1)
            ).start()

    def conclude(k):
        take(mids.at[k, 0:DEPTH - 1], recv2.at[k])
        means = []
        for half in range(2):
            means.append([m / N_SLAB for m in add_up([layer(k, z, half) for z in range(DEPTH)])])
        zs_far[k, 0:8, :] = means[0][0]
        zs_far[k, 8:9, :] = means[0][1]
        zs[k, plane, 0:8, :] = means[1][0]
        zs[k, plane, 8:9, :] = means[1][1]

        def gather(src, peer, core):
            remote(src, zs.at[k, plane], send3.at[k], recv3.at[k], (in_plane(peer), core)).start()

        for peer in far_planes:
            gather(zs_far.at[k], peer, 0)
            gather(zs.at[k, plane], peer, 1)
        gather(zs_far.at[k], plane, 0)

    def statistics(k):
        take(sqs.at[k, 0:DEPTH - 1], recv_sq.at[k])
        primal = jnp.zeros((1, 128), F32)
        dual = jnp.zeros((1, 128), F32)
        for half in range(2):
            mean = consensus_of(k, half)
            layers = [layer(k, z, half) for z in range(DEPTH)]
            if k == 0:
                last = [jnp.zeros((8, 128), F32), jnp.zeros((1, 128), F32)]
            else:
                last = consensus_of(0, half)
                before = [layer(0, z, half) for z in range(DEPTH)]
                layers = [[p - (b - PLANE * z) for p, b, z in zip(new, old, last)] for new, old in zip(layers, before)]
            primal = primal + PLANE * squares([[p / PLANE for p in each] for each in layers], mean)
            dual = dual + squares([mean], last)
        for z in range(DEPTH):
            primal = primal + sqs[k, z]
        return jnp.sum(primal, 1, keepdims=True), N_SLAB * rho * rho * jnp.sum(dual, 1, keepdims=True)

    def gathered(k):
        @pl.when(owner)
        def _():
            take(zs.at[k, 0:PLANE - 1], recv3.at[k])

        @pl.when(jnp.logical_not(owner))
        def _():
            take(zs.at[k], recv3.at[k])

        return from_chunks(zs.at[k])

    lane = lax.broadcasted_iota(jnp.int32, (1, 128), 1)

    send_chunks(0, l1)
    w1 = y + jnp.concatenate([rows3(vd, last, NN), vd], 1)
    for work in eliminate(3, d_ref[...]):
        work()
    inverse = two(s_ref[...])
    fixed = rows3(w1 - rho * M * rows3(w1, inverse, NN), phis(), NT)

    @pl.when(owner)
    def _():
        average(0)

    high, low = two(dot3(inverse, (phi_h[...], phi_l[...]), NT))
    b_h[...] = high
    b_l[...] = low

    @pl.when(owner)
    def _():
        conclude(0)
        primal, dual = statistics(0)
        stats[...] = jnp.where(lane == 0, primal, jnp.where(lane == 2, dual, 0.0))

    z1 = gathered(0)
    l2 = 2.0 * z1 + (fixed - 2.0 * rows3(rows3(z1, phis(), NN), (b_h[...], b_l[...]), NN))
    u1 = l1_ref[...] - z1
    send_chunks(1, l2 + u1)
    lo_ref[:, 0, :] = l2[:, 0:FEATS]
    l1_ref[...] = u1 + l2

    @pl.when(owner)
    def _():
        average(1)
        conclude(1)
        primal, dual = statistics(1)
        res[plane] = jnp.where(lane == 1, primal, jnp.where(lane == 3, dual, stats[...]))
        for peer in far_planes:
            for core in range(2):
                remote(res.at[plane], res.at[plane], send_res.at[0], recv_res.at[0], (in_plane(peer), core)).start()
        remote(res.at[plane], res.at[plane], send_res.at[0], recv_res.at[0], (slab, 0)).start()

    z2 = gathered(1)
    du_ref[:, 0, :] = (l1_ref[...] - z2)[:, 0:FEATS]
    co_ref[...] = z2[:, 0:FEATS]

    @pl.when(owner)
    def _():
        take(res.at[0:PLANE - 1], recv_res.at[0])

    @pl.when(jnp.logical_not(owner))
    def _():
        take(res, recv_res.at[0])

    total = functools.reduce(jnp.add, [res[i] for i in range(PLANE)])
    total = jnp.sqrt(total / (N_SLAB * R * FEATS))
    rh_ref[...] = jnp.concatenate([total[:, 0:2], total[:, 2:4]], 0)

    @pl.when(owner)
    def _():
        for k in range(2):
            take(outs.at[k, 0:PLANE - 1], send1.at[k])
            take(mids.at[k, 0:DEPTH - 1], send2.at[k])
            take(sqs.at[k, 0:DEPTH - 1], send_sq.at[k])
            take(ins.at[k, 0:2 * PLANE - 1], send3.at[k])
        take(sent.at[0:2 * PLANE - 1], send_res.at[0])

    @pl.when(jnp.logical_not(owner))
    def _():
        for k in range(2):
            take(outs.at[k], send1.at[k])


def put_out(*refs):
    sems = refs[-1]
    copies = [pltpu.make_async_copy(refs[i], refs[4 + i], sems.at[i]) for i in range(4)]
    for copy in copies:
        copy.start()
    for copy in copies:
        copy.wait()


def shards(states, inputs, targets):
    vmem = pl.BlockSpec(memory_space=pltpu.VMEM)
    dma = pltpu.SemaphoreType.DMA
    f32 = lambda *shape: pltpu.VMEM(shape, F32)
    half = lambda *shape: pltpu.VMEM(shape, BF16)
    results = (
        jax.ShapeDtypeStruct((HALF, 1, FEATS), F32),
        jax.ShapeDtypeStruct((HALF, 1, FEATS), F32),
        jax.ShapeDtypeStruct((HALF, FEATS), F32),
        jax.ShapeDtypeStruct((2, 2), F32),
    )
    whole = pl.BlockSpec(memory_space=pl.ANY)
    packed = jnp.concatenate([states, targets], 0)
    operators, duals, consensus, history = pl.pallas_call(
        kernel,
        out_shape=results,
        in_specs=[vmem] * 2,
        out_specs=(vmem,) * 4,
        scratch_shapes=[
            f32(2 * R, MINE), f32(1, MINE),
            f32(WIDE, M), half(WIDE, M), half(WIDE, M), f32(M, M), f32(128, 128), half(2, 384, M),
            half(M, WIDE), half(M, WIDE), f32(HALF, WIDE),
            f32(2, PLANE, 9, 128), f32(2, 2 * PLANE, 9, 128), f32(2, DEPTH, 18, 128), f32(2, DEPTH, 1, 128),
            f32(2, PLANE, 9, 128), f32(2, 9, 128), f32(PLANE, 1, 128), f32(2 * PLANE, 1, 128), f32(1, 128),
            dma((4,)), dma((2,)), dma((2,)), dma((2,)), dma((2,)), dma((2,)), dma((2,)), dma((2,)), dma((2,)), dma((1,)), dma((1,)),
        ],
        compiler_params=pltpu.CompilerParams(
            collective_id=0, has_side_effects=True, vmem_limit_bytes=48 * 1024 * 1024
        ),
        name="consensus",
    )(packed, inputs.reshape(1, MINE))
    operators, duals, consensus, history = pl.pallas_call(
        put_out,
        out_shape=results,
        in_specs=[vmem] * 4,
        out_specs=(whole,) * 4,
        scratch_shapes=[dma((4,))],
        compiler_params=pltpu.CompilerParams(vmem_limit_bytes=1024 * 1024),
        name="put_out",
    )(operators, duals, consensus, history)
    return operators.transpose(1, 0, 2), duals.transpose(1, 0, 2), consensus, history


def solution(mesh):
    return jax.shard_map(
        shards,
        mesh=mesh,
        in_specs=(P(None, ("slab", "feat")), P(("slab", "feat")), P(None, ("slab", "feat"))),
        out_specs=(P("slab", "feat", None), P("slab", "feat", None), P("feat", None), P()),
        check_vma=False,
    )
```

```python
import functools

import jax
import jax.numpy as jnp
from jax import lax
from jax.experimental import pallas as pl
from jax.experimental.pallas import tpu as pltpu
from jax.sharding import PartitionSpec as P

F32, BF16 = jnp.float32, jnp.bfloat16
NN = (((1,), (0,)), ((), ()))
NT = (((1,), (1,)), ((), ()))
TN = (((0,), (0,)), ((), ()))
MESH = pl.DeviceIdType.MESH

R = 40
HALF = 20
FEATS = 862
WIDE = 896
PLANE = 16
DEPTH = 8
N_SLAB = 128
M = 512
MINE = 256
rho = 1.0


def dot(a, b, dims):
    return lax.dot_general(a, b, dims, preferred_element_type=F32)


def two(a):
    high = a.astype(BF16)
    return high, (a - high.astype(F32)).astype(BF16)


def dot3(a, b, dims):
    (ah, al), (bh, bl) = a, b
    return dot(ah, bh, dims) + (dot(ah, bl, dims) + dot(al, bh, dims))


def left3(a):
    high, low = two(a)
    return jnp.concatenate([high, low, high], 1)


def right3(b):
    high, low = two(b)
    return jnp.concatenate([high, high, low], 0)


def rows3(a, b, dims):
    rows, pad = a.shape[0], -a.shape[0] % 8
    if pad:
        a = jnp.concatenate([a, jnp.zeros((pad, a.shape[1]), F32)], 0)
    tall = rows + pad
    high = a.astype(BF16).astype(F32)
    both = jnp.concatenate([high, a - high], 0).astype(BF16)
    first = dot(both, b[0], dims)
    return (first[0:tall] + (first[tall:] + dot(high.astype(BF16), b[1], dims)))[0:rows]


def three(a):
    high = a.astype(BF16).astype(F32)
    rest = a - high
    mid = rest.astype(BF16).astype(F32)
    return high, mid, rest - mid


def stacks(x, u):
    def left_of(h, m, l):
        return [h, h, m, h, l, m]

    def right_of(h, m, l):
        return [h, m, h, l, h, m]

    xs, ss, us = three(x), three(x * x), three(u)
    halves = tuple(0.5 * s for s in ss)
    ends = [jnp.ones_like(u), jnp.zeros_like(u)]
    cat = lambda parts: jnp.concatenate(parts, 0).astype(BF16)
    return (
        cat(left_of(*xs)),
        cat(right_of(*xs)),
        cat(left_of(*halves) + left_of(*us) + ends),
        cat(right_of(*ss) + right_of(*us) + ends),
    )


def kernel_block(a, b):
    g = dot(a[0], b[1], TN)
    return g + dot(a[2], b[3], TN) + 0.5 * (g * g)


def add_diagonal(block):
    row = lax.broadcasted_iota(jnp.int32, block.shape, 0)
    col = lax.broadcasted_iota(jnp.int32, block.shape, 1)
    return block + jnp.where(row == col, rho * M, 0.0)


def invert(a, beside=(), n=128, w=16):
    beside = list(beside)
    tiles, wt = n // 8, w // 8
    lane = lax.broadcasted_iota(jnp.int32, (8, n), 1)
    sub = lax.broadcasted_iota(jnp.int32, (8, n), 0)

    def row_of(x, i):
        return jnp.broadcast_to(x[i:i + 1, :], (8, n))

    a = [a[8 * t:8 * t + 8] for t in range(tiles)]
    for j in range(n // w):
        k0, t0 = w * j, wt * j
        near = [t % tiles for t in range(t0 + wt, t0 + 2 * wt)] if j + 1 < n // w else []
        rest = [t for t in range(tiles) if t not in near and not t0 <= t < t0 + wt]
        inside = (lane >= k0) & (lane < k0 + w)

        def spread(t, k):
            return jnp.broadcast_to(a[t][:, k0 + k:k0 + k + 1], (8, n))

        col = [[spread(t0 + s, k) + 0.0 for s in range(wt)] for k in range(w)]
        ahead = {(t, k): spread(t, k) for k in range(w) for t in near}
        row = [jnp.where(inside, (lane == k0 + 8 * s + sub).astype(F32), a[t0 + s]) for s in range(wt)]
        scale = [None] * wt
        for k in range(w):
            if k == 4 and beside:
                beside.pop(0)()
            s0, i = divmod(k, 8)
            inv = 1.0 / row_of(col[k][s0], i)
            scale[s0] = inv if i == 0 else jnp.where(sub == i, inv, scale[s0])
            off = list(col[k])
            off[s0] = jnp.where(sub == i, 0.0, off[s0])
            for m in range(k + 1, w):
                factor = row_of(col[m][s0], i)
                if m == k + 1:
                    col[m] = [c - (o * factor) * inv for c, o in zip(col[m], off)]
                else:
                    factor = factor * inv
                    col[m] = [c - o * factor for c, o in zip(col[m], off)]
            factor = row_of(row[s0], i) * inv
            row = [r - o * factor for r, o in zip(row, off)]
        row = [r * s for r, s in zip(row, scale)]
        pivots = [row_of(row[k // 8], k % 8) for k in range(w)] if near else []
        for t in near:
            terms = [ahead[t, k] * pivots[k] for k in range(w)]
            while len(terms) > 1:
                terms = [functools.reduce(jnp.add, terms[i:i + 2]) for i in range(0, len(terms), 2)]
            a[t] = jnp.where(inside, 0.0, a[t]) - terms[0]
        old = jnp.concatenate([a[t] for t in rest], 0)
        old_h, old_l = two(old)
        new_h, new_l = two(jnp.concatenate(row, 0))
        gap = [jnp.zeros((m, n), BF16) for m in (k0, n - k0 - w)]

        def padded(x):
            return jnp.concatenate([p for p in (gap[0], x, gap[1]) if p.shape[0]], 0)

        high, low = padded(new_h), padded(new_l)
        change = dot(jnp.concatenate([old_h, old_l, old_h], 1), jnp.concatenate([high, high, low], 0), NN)
        for i, t in enumerate(rest):
            a[t] = jnp.where(inside, 0.0, a[t]) - change[8 * i:8 * i + 8]
        for s in range(wt):
            a[t0 + s] = row[s]
    for work in beside:
        work()
    return jnp.concatenate(a, 0)


def write_features(phi_ref, x_ref, u, at):
    cols = pl.ds(at, MINE)
    phi_ref[0:R, cols] = x_ref[...]
    off = R
    for i in range(R):
        phi_ref[off:off + R - i, cols] = x_ref[i:i + 1, :] * x_ref[i:R, :]
        off += R - i
    phi_ref[off:off + 1, cols] = u
    phi_ref[off + 1:off + 2, cols] = jnp.ones_like(u)
    phi_ref[off + 2:WIDE, cols] = jnp.zeros((WIDE - FEATS, MINE), F32)


def to_chunks(whole, out_ref):
    def piece(r, n, c):
        return whole[r:r + n, 128 * c:128 * c + 128]

    for c in range(7):
        out_ref[2 * c, 0:8, :] = piece(0, 8, c)
        out_ref[2 * c + 1, 0:8, :] = piece(8, 8, c)
    out_ref[14, 0:8, :] = jnp.concatenate([piece(16, 4, 0), piece(16, 4, 1)], 0)
    out_ref[15, 0:8, :] = jnp.concatenate([piece(16, 4, 2), piece(16, 4, 3)], 0)
    for i in range(12):
        out_ref[i, 8:9, :] = piece(16 + i % 4, 1, 4 + i // 4)
    for i in range(12, 16):
        out_ref[i, 8:9, :] = jnp.zeros((1, 128), F32)


def from_chunks(ref):
    columns = []
    for c in range(7):
        if c < 4:
            last = ref[14 + c // 2, 4 * (c % 2):4 * (c % 2) + 4, :]
        else:
            last = jnp.concatenate([ref[4 * (c - 4) + i, 8:9, :] for i in range(4)], 0)
        columns.append(jnp.concatenate([ref[2 * c, 0:8, :], ref[2 * c + 1, 0:8, :], last], 0))
    return jnp.concatenate(columns, 1)


def rows_sum(main, ext):
    return jnp.sum(main, 0, keepdims=True) + ext


def kernel(
    near_ref, u_ref, lo_ref, du_ref, co_ref, rh_ref,
    far_ref, uo, phi, phi_h, phi_l, s_ref, d_ref, p_ref, b_h, b_l, l1_ref,
    outs, ins, mids, sqs, zs, zs_far, res, sent, stats,
    pair_sems, send1, recv1, send2, recv2, send3, recv3, send_sq, recv_sq, send_res, recv_res,
):
    (x_ref, t_ref), (xo, to) = ([ref.at[0:R], ref.at[R:2 * R]] for ref in (near_ref, far_ref))
    slab = lax.axis_index("slab")
    feat = lax.axis_index("feat")
    plane = lax.rem(slab, PLANE)
    depth = lax.div(slab, PLANE)
    line, spot = lax.div(plane, 4), lax.rem(plane, 4)
    other = 1 - feat
    owner = feat == 1
    steps = sorted(((dy, dx) for dy in range(4) for dx in range(4) if dy or dx), key=lambda d: -sum(min(v, 4 - v) for v in d))
    far_planes = [4 * lax.rem(line + dy, 4) + lax.rem(spot + dx, 4) for dy, dx in steps]
    far_depths = [lax.rem(depth + d, DEPTH) for d in (4, 3, 5, 2, 6, 1, 7)]

    def in_plane(i):
        return depth * PLANE + i

    def in_depth(i):
        return i * PLANE + plane

    barrier = pltpu.get_barrier_semaphore()

    def greet(s, f):
        pl.semaphore_signal(barrier, inc=1, device_id=(s, f), device_id_type=MESH)

    greet(slab, other)
    for peer in far_planes:
        greet(in_plane(peer), 1)

    @pl.when(owner)
    def _():
        for peer in far_planes:
            greet(in_plane(peer), 0)
        for peer in far_depths:
            greet(in_depth(peer), 1)

    u_own = u_ref[...]
    own = stacks(x_ref[...], u_own)
    s_ref[0:MINE, 0:MINE] = add_diagonal(kernel_block(own, own))

    pair = [
        pltpu.make_async_remote_copy(
            src_ref=src, dst_ref=dst, send_sem=pair_sems.at[i], recv_sem=pair_sems.at[2 + i],
            device_id=(slab, other), device_id_type=MESH,
        )
        for i, (src, dst) in enumerate(((near_ref, far_ref), (u_ref, uo)))
    ]
    def meet():
        pl.semaphore_wait(barrier, PLANE + feat * (PLANE + DEPTH - 2))
        for copy in pair:
            copy.start()

    def block(r, c):
        return s_ref[128 * r:128 * r + 128, 128 * c:128 * c + 128]

    def next_block(kb, inverse):
        ahead = dot(left3(inverse), right3(block(kb, kb + 1)), NN)
        return block(kb + 1, kb + 1) - dot(left3(block(kb + 1, kb)), right3(ahead), NN)

    def eliminate(kb, inverse):
        rows = slice(128 * kb, 128 * kb + 128)

        def pivots():
            left = left3(inverse)
            new = jnp.concatenate(
                [inverse if c == kb else dot(left, right3(block(kb, c)), NN) for c in range(4)], 1
            )
            s_ref[rows, :] = new
            p_ref[kb % 2] = right3(new)

        def update(rb):
            at = slice(128 * rb, 128 * rb + 128)
            change = dot(left3(block(rb, kb)), p_ref[kb % 2], NN)
            for c in range(4):
                old = 0.0 if c == kb else block(rb, c)
                s_ref[at, 128 * c:128 * c + 128] = old - change[:, 128 * c:128 * c + 128]

        return [pivots] + [functools.partial(update, (kb + i) % 4) for i in range(1, 4)]

    def far_blocks():
        u_far = uo[...]
        own = stacks(x_ref[...], u_ref[...])
        far = stacks(xo[...], u_far)
        s_ref[0:MINE, MINE:M] = kernel_block(own, far)
        s_ref[MINE:M, 0:MINE] = kernel_block(far, own)
        s_ref[MINE:M, MINE:M] = add_diagonal(kernel_block(far, far))

    def split_features(i):
        part = slice(224 * i, 224 * i + 224)
        phi_h[part], phi_l[part] = two(phi[part])

    inverse = invert(block(0, 0), [meet, lambda: write_features(phi, x_ref, u_ref[...], 0)])
    pivot = next_block(0, inverse)
    for copy in pair:
        copy.wait()
    inverse = invert(pivot, [far_blocks] + eliminate(0, inverse) + [lambda: write_features(phi, xo, uo[...], MINE)])
    pivot = next_block(1, inverse)
    inverse = invert(pivot, eliminate(1, inverse) + [functools.partial(split_features, i) for i in range(4)])
    pivot = next_block(2, inverse)

    def phis():
        return phi_h[...], phi_l[...]

    first = feat == 0
    rest_rows = slice(0, 384)
    kept = {}

    def solve_rest():
        targets = jnp.concatenate(
            [jnp.where(first, t[0:HALF, :], t[HALF:R, :]) for t in (t_ref, to)], 1
        )
        left = rows3(targets[:, rest_rows], two(s_ref[rest_rows, :]), NN)
        kept["v"] = targets[:, 384:M] - left[:, 384:M]
        kept["y"] = jnp.concatenate([left[:, rest_rows], jnp.zeros((HALF, 128), F32)], 1)

    def apply_rest():
        kept["ly"] = rows3(kept["y"], phis(), NT)

    def last_features():
        kept["last"] = two(s_ref[384:M, rest_rows])
        kept["g3"] = two(
            dot3(kept["last"], (phi_h[:, rest_rows], phi_l[:, rest_rows]), NT) + phi[:, 384:M].T
        )

    inverse = invert(pivot, eliminate(2, inverse) + [solve_rest, apply_rest, last_features])
    v, y, ly, last, g3 = (kept[name] for name in ("v", "y", "ly", "last", "g3"))
    vd = rows3(v, two(inverse), NN)
    l1 = ly + rows3(vd, g3, NN)
    l1_ref[...] = l1
    d_ref[...] = inverse

    def remote(src, dst, send, recv, device):
        return pltpu.make_async_remote_copy(
            src_ref=src, dst_ref=dst, send_sem=send, recv_sem=recv, device_id=device, device_id_type=MESH
        )

    def take(ref, sem):
        pltpu.make_async_copy(ref, ref, sem).wait()

    def send_chunks(k, whole):
        to_chunks(whole, outs.at[k])

        def scatter(peer):
            remote(
                outs.at[k, peer], ins.at[k, feat * PLANE + plane], send1.at[k], recv1.at[k], (in_plane(peer), 1)
            ).start()

        for peer in far_planes:
            scatter(peer)

        @pl.when(owner)
        def _():
            ins[k, PLANE + plane] = outs[k, plane]

        @pl.when(jnp.logical_not(owner))
        def _():
            scatter(plane)

    def parts(ref, *at):
        return [ref[(*at, slice(0, 8))], ref[(*at, slice(8, 9))]]

    def add_up(pieces):
        return [functools.reduce(jnp.add, [p[i] for p in pieces]) for i in range(2)]

    def squares(pieces, mean):
        total = [jnp.zeros((8, 128), F32), jnp.zeros((1, 128), F32)]
        for piece in pieces:
            for i in range(2):
                gap = piece[i] - mean[i]
                total[i] = total[i] + gap * gap
        return jnp.sum(total[0], 0, keepdims=True) + total[1]

    def consensus_of(k, half):
        return parts(zs, k, plane) if half else parts(zs_far, k)

    def layer(k, z, half):
        return [mids[k, z, 8 * half:8 * half + 8, :], mids[k, z, 16 + half:17 + half, :]]

    def average(k):
        take(ins.at[k, 0:2 * PLANE - 1], recv1.at[k])
        totals = [add_up([parts(ins, k, PLANE * half + s) for s in range(PLANE)]) for half in range(2)]
        for half in range(2):
            mids[k, depth, 8 * half:8 * half + 8, :] = totals[half][0]
            mids[k, depth, 16 + half:17 + half, :] = totals[half][1]
        for peer in far_depths:
            remote(
                mids.at[k, depth], mids.at[k, depth], send2.at[k], recv2.at[k], (in_depth(peer), 1)
            ).start()
        spread = jnp.zeros((1, 128), F32)
        for half in range(2):
            mean = totals[half]
            operators = [parts(ins, k, PLANE * half + s) for s in range(PLANE)]
            if k == 1:
                last = consensus_of(0, half)
                before = [parts(ins, 0, PLANE * half + s) for s in range(PLANE)]
                operators = [[p - (b - z) for p, b, z in zip(new, old, last)] for new, old in zip(operators, before)]
                mean = add_up(operators)
            spread = spread + squares(operators, [m / PLANE for m in mean])
        sqs[k, depth] = spread
        for peer in far_depths:
            remote(
                sqs.at[k, depth], sqs.at[k, depth], send_sq.at[k], recv_sq.at[k], (in_depth(peer), 1)
            ).start()

    def conclude(k):
        take(mids.at[k, 0:DEPTH - 1], recv2.at[k])
        means = []
        for half in range(2):
            means.append([m / N_SLAB for m in add_up([layer(k, z, half) for z in range(DEPTH)])])
        zs_far[k, 0:8, :] = means[0][0]
        zs_far[k, 8:9, :] = means[0][1]
        zs[k, plane, 0:8, :] = means[1][0]
        zs[k, plane, 8:9, :] = means[1][1]

        def gather(src, peer, core):
            remote(src, zs.at[k, plane], send3.at[k], recv3.at[k], (in_plane(peer), core)).start()

        for peer in far_planes:
            gather(zs_far.at[k], peer, 0)
            gather(zs.at[k, plane], peer, 1)
        gather(zs_far.at[k], plane, 0)

    def statistics(k):
        take(sqs.at[k, 0:DEPTH - 1], recv_sq.at[k])
        primal = jnp.zeros((1, 128), F32)
        dual = jnp.zeros((1, 128), F32)
        for half in range(2):
            mean = consensus_of(k, half)
            layers = [layer(k, z, half) for z in range(DEPTH)]
            if k == 0:
                last = [jnp.zeros((8, 128), F32), jnp.zeros((1, 128), F32)]
            else:
                last = consensus_of(0, half)
                before = [layer(0, z, half) for z in range(DEPTH)]
                layers = [[p - (b - PLANE * z) for p, b, z in zip(new, old, last)] for new, old in zip(layers, before)]
            primal = primal + PLANE * squares([[p / PLANE for p in each] for each in layers], mean)
            dual = dual + squares([mean], last)
        for z in range(DEPTH):
            primal = primal + sqs[k, z]
        return jnp.sum(primal, 1, keepdims=True), N_SLAB * rho * rho * jnp.sum(dual, 1, keepdims=True)

    def gathered(k):
        @pl.when(owner)
        def _():
            take(zs.at[k, 0:PLANE - 1], recv3.at[k])

        @pl.when(jnp.logical_not(owner))
        def _():
            take(zs.at[k], recv3.at[k])

        return from_chunks(zs.at[k])

    lane = lax.broadcasted_iota(jnp.int32, (1, 128), 1)

    send_chunks(0, l1)
    w1 = y + jnp.concatenate([rows3(vd, last, NN), vd], 1)
    for work in eliminate(3, d_ref[...]):
        work()
    inverse = two(s_ref[...])
    fixed = rows3(w1 - rho * M * rows3(w1, inverse, NN), phis(), NT)

    @pl.when(owner)
    def _():
        average(0)

    high, low = two(dot3(inverse, (phi_h[...], phi_l[...]), NT))
    b_h[...] = high
    b_l[...] = low

    @pl.when(owner)
    def _():
        conclude(0)
        primal, dual = statistics(0)
        stats[...] = jnp.where(lane == 0, primal, jnp.where(lane == 2, dual, 0.0))

    z1 = gathered(0)
    l2 = 2.0 * z1 + (fixed - 2.0 * rows3(rows3(z1, phis(), NN), (b_h[...], b_l[...]), NN))
    u1 = l1_ref[...] - z1
    send_chunks(1, l2 + u1)
    lo_ref[:, 0, :] = l2[:, 0:FEATS]
    l1_ref[...] = u1 + l2

    @pl.when(owner)
    def _():
        average(1)
        conclude(1)
        primal, dual = statistics(1)
        res[plane] = jnp.where(lane == 1, primal, jnp.where(lane == 3, dual, stats[...]))
        for peer in far_planes:
            for core in range(2):
                remote(res.at[plane], res.at[plane], send_res.at[0], recv_res.at[0], (in_plane(peer), core)).start()
        remote(res.at[plane], res.at[plane], send_res.at[0], recv_res.at[0], (slab, 0)).start()

    z2 = gathered(1)
    du_ref[:, 0, :] = (l1_ref[...] - z2)[:, 0:FEATS]
    co_ref[...] = z2[:, 0:FEATS]

    @pl.when(owner)
    def _():
        take(res.at[0:PLANE - 1], recv_res.at[0])

    @pl.when(jnp.logical_not(owner))
    def _():
        take(res, recv_res.at[0])

    total = functools.reduce(jnp.add, [res[i] for i in range(PLANE)])
    total = jnp.sqrt(total / (N_SLAB * R * FEATS))
    rh_ref[...] = jnp.concatenate([total[:, 0:2], total[:, 2:4]], 0)

    @pl.when(owner)
    def _():
        for k in range(2):
            take(outs.at[k, 0:PLANE - 1], send1.at[k])
            take(mids.at[k, 0:DEPTH - 1], send2.at[k])
            take(sqs.at[k, 0:DEPTH - 1], send_sq.at[k])
            take(ins.at[k, 0:2 * PLANE - 1], send3.at[k])
        take(sent.at[0:2 * PLANE - 1], send_res.at[0])

    @pl.when(jnp.logical_not(owner))
    def _():
        for k in range(2):
            take(outs.at[k], send1.at[k])


def put_out(*refs):
    sems = refs[-1]
    copies = [pltpu.make_async_copy(refs[i], refs[4 + i], sems.at[i]) for i in range(4)]
    for copy in copies:
        copy.start()
    for copy in copies:
        copy.wait()


def shards(states, inputs, targets):
    vmem = pl.BlockSpec(memory_space=pltpu.VMEM)
    dma = pltpu.SemaphoreType.DMA
    f32 = lambda *shape: pltpu.VMEM(shape, F32)
    half = lambda *shape: pltpu.VMEM(shape, BF16)
    results = (
        jax.ShapeDtypeStruct((HALF, 1, FEATS), F32),
        jax.ShapeDtypeStruct((HALF, 1, FEATS), F32),
        jax.ShapeDtypeStruct((HALF, FEATS), F32),
        jax.ShapeDtypeStruct((2, 2), F32),
    )
    whole = pl.BlockSpec(memory_space=pl.ANY)
    packed = jnp.concatenate([states, targets], 0)
    operators, duals, consensus, history = pl.pallas_call(
        kernel,
        out_shape=results,
        in_specs=[vmem] * 2,
        out_specs=(vmem,) * 4,
        scratch_shapes=[
            f32(2 * R, MINE), f32(1, MINE),
            f32(WIDE, M), half(WIDE, M), half(WIDE, M), f32(M, M), f32(128, 128), half(2, 384, M),
            half(M, WIDE), half(M, WIDE), f32(HALF, WIDE),
            f32(2, PLANE, 9, 128), f32(2, 2 * PLANE, 9, 128), f32(2, DEPTH, 18, 128), f32(2, DEPTH, 1, 128),
            f32(2, PLANE, 9, 128), f32(2, 9, 128), f32(PLANE, 1, 128), f32(2 * PLANE, 1, 128), f32(1, 128),
            dma((4,)), dma((2,)), dma((2,)), dma((2,)), dma((2,)), dma((2,)), dma((2,)), dma((2,)), dma((2,)), dma((1,)), dma((1,)),
        ],
        compiler_params=pltpu.CompilerParams(
            collective_id=0, has_side_effects=True, vmem_limit_bytes=48 * 1024 * 1024
        ),
        name="consensus",
    )(packed, inputs.reshape(1, MINE))
    operators, duals, consensus, history = pl.pallas_call(
        put_out,
        out_shape=results,
        in_specs=[vmem] * 4,
        out_specs=(whole,) * 4,
        scratch_shapes=[dma((4,))],
        compiler_params=pltpu.CompilerParams(vmem_limit_bytes=1024 * 1024),
        name="put_out",
    )(operators, duals, consensus, history)
    return operators.transpose(1, 0, 2), duals.transpose(1, 0, 2), consensus, history


def solution(mesh):
    return jax.shard_map(
        shards,
        mesh=mesh,
        in_specs=(P(None, ("slab", "feat")), P(("slab", "feat")), P(None, ("slab", "feat"))),
        out_specs=(P("slab", "feat", None), P("slab", "feat", None), P("feat", None), P()),
        check_vma=False,
    )
```
